32 devices in a mesh: lat: 8 (over z, x), lon: 4 (over y, core).
Axes of the slice: x: 2, y: 2, z: 4, core: 2. Of those that a mesh axis runs over, the one named last changes fastest.
Arguments:
- fields: float32 [8, 8, 128, 512], P(None, None, 'lat', 'lon'), may hold values from -6 to 6
- ocean_mask: int32 [128, 4], replicated, may hold values from 0 to 1, as said below
- scale_table: float32 [16], replicated, may hold values from 0.5 to 4
- offset_table: float32 [16], replicated, may hold values from -4 to 4
- scale_index: int32 [8], replicated, may hold values from 0 to 15
- offset_index: int32 [8], replicated, may hold values from 0 to 15
Outputs:
- history: float32 [8, 8, 128, 512], P(None, 'lat', 'lon')
- record_range: float32 [2, 8, 8], P(None, None, 'lat')
The draws below stay inside these ranges and needn't reach their ends.
Inputs may be any that keep to these rules, and one draw needn't show every extreme that they name: `ocean_mask`: each device's block of 16 rows and 128 longitudes holds at least half of 12 (rounded down, and never fewer than one) and at most 12 ocean strips; some block holds exactly 12.
All inputs are finite; a program needn't handle non-finite values.
Results may differ from the reference program's by a relative error of at most 0.00007.
Values sent between devices are 32-bit elements; how exact they have to be, the bound alone decides.
A program may use at most 64 MiB of HBM per device.

```python
import math
import jax
import jax.numpy as jnp

FIELDS = 8
TABLE = 16
LAT_DEV = 16
LON_DEV = 128
STRIP = 128
LEVELS = 8
NLAT = 128
NLON = 512
NSTRIP = 4
MAX_LIVE = 12


def draw_ocean_mask(key, part):
    strips_row = LON_DEV // STRIP
    per_block = LAT_DEV * strips_row
    blocks_lat = NLAT // LAT_DEV
    blocks_lon = NSTRIP // strips_row
    total_blocks = blocks_lat * blocks_lon
    count_key = jax.random.fold_in(key, 11)
    full_key = jax.random.fold_in(key, 12)
    score_key = jax.random.fold_in(key, 13)
    fewest = max(1, MAX_LIVE // 2)
    counts = jax.random.randint(count_key, (total_blocks,), fewest, MAX_LIVE + 1)
    full_block = jax.random.randint(full_key, (), 0, total_blocks)
    counts = jnp.where(jnp.arange(total_blocks) == full_block, MAX_LIVE, counts)
    scores = jax.random.randint(score_key, (total_blocks, per_block), 0, 1 << 20) * per_block
    scores = scores + jnp.arange(per_block)[None, :]
    ranks = jnp.argsort(jnp.argsort(scores, axis=1), axis=1)
    ocean = (ranks < counts[:, None]).astype(jnp.int32)
    ocean = ocean.reshape(blocks_lat, blocks_lon, LAT_DEV, strips_row).transpose(0, 2, 1, 3)
    return ocean.reshape(NLAT, NSTRIP)


def with_ends(entries, own_key, smallest, top_value):
    dims = entries.shape
    place = [jax.random.randint(jax.random.fold_in(own_key, axis), (), 0, dims[axis]) for axis in range(len(dims))]
    entries = entries.at[tuple(place)].set(smallest)
    longest = dims.index(max(dims))
    place[longest] = (place[longest] + 1) % dims[longest]
    return entries.at[tuple(place)].set(top_value)


def levels(own_key, extent, split, low, largest):
    loudness, own = 1.0, jax.random.fold_in(own_key, 6)
    for dim, blocks in split:
        heights = jnp.exp(jax.random.uniform(jax.random.fold_in(own, dim), (blocks,), jnp.float32, low / len(split), largest / len(split)))
        loudness = loudness * jnp.repeat(heights, extent[dim] // blocks).reshape([-1 if axis == dim else 1 for axis in range(len(extent))])
    return loudness


def bell_draw(own_key, dims, scale, limit, split=(), held_as=jnp.bfloat16):
    drawn = jax.random.normal(own_key, dims, jnp.float32) * scale
    if len(split) > 0:
        drawn = levels(own_key, dims, split, -0.22, 0.18) * drawn
    return jnp.clip(drawn, min=-limit, max=limit).astype(held_as)


def setup_inputs(seed: int = 0) -> dict:
    splits = jax.random.split(jax.random.key(seed), 7)
    return {
        "fields": bell_draw(splits[0], (FIELDS, LEVELS, NLAT, NLON), 1.0, 6.0, ((2, 8), (3, 4)), jnp.float32),
        "ocean_mask": draw_ocean_mask(jax.random.fold_in(splits[6], 71), 0),
        "scale_table": jnp.clip(jnp.exp(jax.random.uniform(splits[2], (TABLE,), jnp.float32, math.log(0.5), math.log(4.0))), 0.5, 4.0),
        "offset_table": bell_draw(splits[3], (TABLE,), 1.0, 4.0, (), jnp.float32),
        "scale_index": with_ends(jax.random.randint(splits[4], (FIELDS,), 0, TABLE), jax.random.fold_in(splits[4], 1), 0, TABLE - 1).astype(jnp.int32),
        "offset_index": with_ends(jax.random.randint(splits[5], (FIELDS,), 0, TABLE), jax.random.fold_in(splits[5], 1), 0, TABLE - 1).astype(jnp.int32),
    }


def reference(fields, ocean_mask, scale_table, offset_table, scale_index, offset_index):
    scales = scale_table[scale_index].astype(jnp.float32)
    offsets = offset_table[offset_index].astype(jnp.float32)
    ocean_cells = jnp.repeat(ocean_mask, STRIP, axis=1) > 0
    packed = (fields - offsets[:, None, None, None]) * scales[:, None, None, None]
    history = jnp.where(ocean_cells[None, None], packed, jnp.zeros_like(packed))
    highest = jnp.max(jnp.where(ocean_cells[None, None], packed, -jnp.inf), axis=(2, 3))
    lowest = jnp.min(jnp.where(ocean_cells[None, None], packed, jnp.inf), axis=(2, 3))
    return history, jnp.stack([highest, lowest])
```

```python
import functools

import jax
import jax.numpy as jnp
from jax import lax
from jax.experimental import pallas as pl
from jax.experimental.pallas import tpu as pltpu
from jax.sharding import PartitionSpec as P

STRIP = 128
MAX_LIVE = 12
MESH = pl.DeviceIdType.MESH


def loop(low, high, body):
    def step(n, carry):
        body(n)
        return carry

    lax.fori_loop(low, high, step, 0)


def exchange(
    dims, mask_hbm, scale_table_hbm, offset_table_hbm, scale_index_hbm, offset_index_hbm, x_hbm,
    out, rng, *scratch,
):
    fields, levels, rows, lat_count, lon_count = dims
    xs, (
        mask, scale_table, offset_table, scale_index, offset_index,
        send, recv, stage, part, mine, first_stats, last_stats,
        x_sem, in_sem, send_sem, recv_sem, stat_send, stat_recv, last_send, last_recv,
    ) = scratch[:levels], scratch[levels:]
    slab = lat_count // lon_count
    planes = lat_count // slab
    sources = slab * lon_count
    slots = send.shape[1]
    lat_pos = lax.axis_index("lat")
    lon_pos = lax.axis_index("lon")
    plane = lat_pos // slab
    here = lax.rem(lat_pos, slab) * lon_count + lon_pos
    lower = plane < planes // 2
    home = plane == lon_pos

    def order(n):
        block, i = n // slab, n % slab
        up = lax.rem(plane + 1 + block, planes)
        down = jnp.where(block < plane, block, jnp.where(block + 1 < planes, block + 1, plane))
        return jnp.where(lower, up, down) * slab + lax.rem(lat_pos + i, slab)

    levels_in_order = [order(n) for n in range(levels)]

    barrier = pltpu.get_barrier_semaphore()

    def greet(source):
        lat, lon = lon_pos * slab + source // lon_count, lax.rem(source, lon_count)

        @pl.when(jnp.logical_not(jnp.logical_and(lat == lat_pos, lon == lon_pos)))
        def _():
            pl.semaphore_signal(barrier, inc=1, device_id=(lat, lon), device_id_type=MESH)

    def greet_lon(step):
        pl.semaphore_signal(
            barrier, inc=1, device_id=(lat_pos, lax.rem(lon_pos + step, lon_count)), device_id_type=MESH
        )

    smalls = [
        pltpu.make_async_copy(src, dst, in_sem.at[n])
        for n, (src, dst) in enumerate([
            (mask_hbm, mask), (scale_table_hbm, scale_table), (offset_table_hbm, offset_table),
            (scale_index_hbm, scale_index), (offset_index_hbm, offset_index),
        ])
    ]
    loads = [
        pltpu.make_async_copy(x_hbm.at[:, levels_in_order[n]], xs[n], x_sem.at[n]) for n in range(levels)
    ]
    loop(0, sources, greet)
    for copy in smalls:
        copy.start()
    for copy in loads:
        copy.start()
    loop(1, lon_count, greet_lon)
    for copy in smalls:
        copy.wait()

    seen = []
    total = jnp.int32(0)
    for r in range(rows):
        total = total + mask[lon_pos, lat_pos * rows + r]
        seen.append(total)
    picks = []
    for k in range(slots):
        slot = jnp.minimum(k, total - 1)
        pick = jnp.int32(0)
        for r in range(rows - 1):
            pick = pick + (seen[r] <= slot).astype(jnp.int32)
        picks.append(pick)

    which = lax.broadcasted_iota(jnp.int32, (fields, STRIP), 0)
    scales = jnp.zeros((fields, STRIP), jnp.float32)
    offsets = jnp.zeros((fields, STRIP), jnp.float32)
    for f in range(fields):
        scales = jnp.where(which == f, scale_table[scale_index[f]], scales)
        offsets = jnp.where(which == f, offset_table[offset_index[f]], offsets)

    for n in range(levels):
        loads[n].wait()
        lines = xs[n].reshape(fields * rows, STRIP)
        high = None
        for k in range(slots):
            strip = lines[pl.ds(picks[k], fields, stride=rows), :]
            packed = (strip - offsets) * scales
            send[n, k] = packed
            high = packed if k == 0 else jnp.maximum(high, packed)
            low = -packed if k == 0 else jnp.maximum(low, -packed)
        level = levels_in_order[n]
        part[pl.ds(pl.multiple_of(level * fields, fields), fields), :] = high
        part[pl.ds(pl.multiple_of((levels + level) * fields, fields), fields), :] = low

    for j in range(mine.shape[0]):
        tile = part[j * STRIP:(j + 1) * STRIP, :].T
        mine[j] = jnp.max(tile, axis=0, keepdims=True)

    pl.semaphore_wait(barrier, levels + lon_count - 1 - home.astype(jnp.int32))

    def is_self(level):
        return jnp.logical_and(level == lat_pos, home)

    def tell(level):
        return pltpu.make_async_remote_copy(
            src_ref=mine,
            dst_ref=first_stats.at[here],
            send_sem=stat_send.at[level],
            recv_sem=stat_recv.at[here],
            device_id=(level, plane),
            device_id_type=MESH,
        )

    def remote(n):
        return pltpu.make_async_remote_copy(
            src_ref=send.at[n],
            dst_ref=recv.at[here],
            send_sem=send_sem.at[n],
            recv_sem=recv_sem.at[here],
            device_id=(levels_in_order[n], plane),
            device_id_type=MESH,
        )

    def when_remote(level, body):
        pl.when(jnp.logical_not(is_self(level)))(body)

    loop(0, levels, lambda level: when_remote(level, lambda: tell(level).start()))
    for n in range(levels):
        when_remote(levels_in_order[n], lambda n=n: remote(n).start())

    @pl.when(home)
    def _():
        first_stats[here] = mine[...]

    for n in range(levels - slab, levels):

        @pl.when(is_self(levels_in_order[n]))
        def _(n=n):
            recv[here] = send[n]

    def not_me(source, body):
        pl.when(jnp.logical_not(jnp.logical_and(home, source == here)))(body)

    loop(0, sources, lambda source: not_me(source, lambda: pltpu.make_async_copy(
        first_stats.at[source], first_stats.at[source], stat_recv.at[source]).wait()))
    last_stats[lon_pos] = jnp.max(first_stats[...], axis=0)

    def share(step):
        return pltpu.make_async_remote_copy(
            src_ref=last_stats.at[lon_pos],
            dst_ref=last_stats.at[lon_pos],
            send_sem=last_send.at[step],
            recv_sem=last_recv.at[step],
            device_id=(lat_pos, lax.rem(lon_pos + step, lon_count)),
            device_id_type=MESH,
        )

    loop(1, lon_count, lambda n: share(n).start())

    per_field = (slab * rows) * lon_count

    for b in range(lon_count):
        for i in range(slab):
            source = i * lon_count + b
            not_me(source, lambda source=source: pltpu.make_async_copy(
                recv.at[source], recv.at[source], recv_sem.at[source]).wait())
            stage[source] = recv[source]
            rank = jnp.int32(0)
            for r in range(rows):
                live = mask[b, (lon_pos * slab + i) * rows + r]
                strip = stage[source, jnp.minimum(rank, slots - 1)]
                strip = jnp.where(live > 0, strip, 0.0)
                line = i * rows + r
                start = (line // 8 * lon_count + b) * 8 + line % 8
                out[pl.ds(start, fields, stride=per_field), :] = strip
                rank = rank + live

    loop(1, lon_count, lambda n: share(n).wait())
    for end in range(2):
        first = (end * levels + lat_pos) * fields
        best = jnp.max(last_stats[:, first // STRIP], axis=0)
        best = jnp.broadcast_to(best, (8, STRIP))
        own = pltpu.roll(best, lax.rem(STRIP - lax.rem(first, STRIP), STRIP), 1)
        own = own[:1, :fields]
        rng[end] = own if end == 0 else -own

    for n in range(levels):
        when_remote(levels_in_order[n], lambda n=n: remote(n).wait_send())
    loop(0, levels, lambda level: when_remote(level, lambda: tell(level).wait_send()))


def store(history, record_range, history_out, record_range_out, sem):
    copies = [
        pltpu.make_async_copy(history, history_out, sem.at[0]),
        pltpu.make_async_copy(record_range, record_range_out, sem.at[1]),
    ]
    for copy in copies:
        copy.start()
    for copy in copies:
        copy.wait()


def per_device(fields, ocean_mask, scale_table, offset_table, scale_index, offset_index):
    nfield, levels, rows, cells = fields.shape
    lat_count = lax.axis_size("lat")
    lon_count = lax.axis_size("lon")
    slab = lat_count // lon_count
    slots = min(MAX_LIVE, rows)
    sources = slab * lon_count
    out_rows = nfield * slab * rows * lon_count
    stat_rows = 2 * levels * nfield // STRIP
    hbm = pl.BlockSpec(memory_space=pltpu.HBM)
    vmem = pl.BlockSpec(memory_space=pltpu.VMEM)
    history, record_range = pl.pallas_call(
        functools.partial(exchange, (nfield, levels, rows, lat_count, lon_count)),
        out_shape=(
            pltpu.VMEM((out_rows, STRIP), jnp.float32),
            pltpu.VMEM((2, 1, nfield), jnp.float32),
        ),
        in_specs=[hbm] * 6,
        out_specs=(vmem, vmem),
        scratch_shapes=[pltpu.VMEM((nfield, rows, STRIP), jnp.float32)] * levels + [
            pltpu.SMEM((lon_count, lat_count * rows), jnp.int32),
            pltpu.SMEM(scale_table.shape, jnp.float32),
            pltpu.SMEM(offset_table.shape, jnp.float32),
            pltpu.SMEM(scale_index.shape, jnp.int32),
            pltpu.SMEM(offset_index.shape, jnp.int32),
            pltpu.VMEM((levels, slots, nfield, STRIP), jnp.float32),
            pltpu.VMEM((sources, slots, nfield, STRIP), jnp.float32),
            pltpu.VMEM((sources, slots, nfield, STRIP), jnp.float32),
            pltpu.VMEM((2 * levels * nfield, STRIP), jnp.float32),
            pltpu.VMEM((stat_rows, 1, STRIP), jnp.float32),
            pltpu.VMEM((sources, stat_rows, 1, STRIP), jnp.float32),
            pltpu.VMEM((lon_count, stat_rows, 1, STRIP), jnp.float32),
            pltpu.SemaphoreType.DMA((levels,)),
            pltpu.SemaphoreType.DMA((5,)),
            pltpu.SemaphoreType.DMA((levels,)),
            pltpu.SemaphoreType.DMA((sources,)),
            pltpu.SemaphoreType.DMA((levels,)),
            pltpu.SemaphoreType.DMA((sources,)),
            pltpu.SemaphoreType.DMA((lon_count,)),
            pltpu.SemaphoreType.DMA((lon_count,)),
        ],
        compiler_params=pltpu.CompilerParams(
            collective_id=0, has_side_effects=True
        ),
    )(ocean_mask.T, scale_table, offset_table, scale_index, offset_index, fields)
    history, record_range = pl.pallas_call(
        store,
        out_shape=(
            jax.ShapeDtypeStruct(history.shape, jnp.float32),
            jax.ShapeDtypeStruct(record_range.shape, jnp.float32),
        ),
        in_specs=[vmem, vmem],
        out_specs=(hbm, hbm),
        scratch_shapes=[pltpu.SemaphoreType.DMA((2,))],
        compiler_params=pltpu.CompilerParams(vmem_limit_bytes=1 << 20),
    )(
        pltpu.with_memory_space_constraint(history, pltpu.VMEM),
        pltpu.with_memory_space_constraint(record_range, pltpu.VMEM),
    )
    history = history.reshape(nfield, slab * rows // 8, lon_count, 8, STRIP)
    history = history.transpose(0, 1, 3, 2, 4)
    return history.reshape(nfield, 1, slab * rows, lon_count * STRIP), record_range.reshape(2, nfield, 1)


def solution(mesh):
    return jax.shard_map(
        per_device,
        mesh=mesh,
        in_specs=(P(None, None, "lat", "lon"), P(), P(), P(), P(), P()),
        out_specs=(P(None, "lat", "lon", None), P(None, None, "lat")),
        check_vma=False,
    )
```

```python
import functools

import jax
import jax.numpy as jnp
from jax import lax
from jax.experimental import pallas as pl
from jax.experimental.pallas import tpu as pltpu
from jax.sharding import PartitionSpec as P

STRIP = 128
MAX_LIVE = 12
MESH = pl.DeviceIdType.MESH


def loop(low, high, body):
    def step(n, carry):
        body(n)
        return carry

    lax.fori_loop(low, high, step, 0)


def exchange(
    dims, mask_hbm, scale_table_hbm, offset_table_hbm, scale_index_hbm, offset_index_hbm, x_hbm,
    out, rng, *scratch,
):
    fields, levels, rows, lat_count, lon_count = dims
    xs, (
        mask, scale_table, offset_table, scale_index, offset_index,
        send, recv, stage, part, mine, first_stats, last_stats,
        x_sem, in_sem, send_sem, recv_sem, stat_send, stat_recv, last_send, last_recv, token,
    ) = scratch[:levels], scratch[levels:]
    slab = lat_count // lon_count
    planes = lat_count // slab
    sources = slab * lon_count
    slots = send.shape[1]
    lat_pos = lax.axis_index("lat")
    lon_pos = lax.axis_index("lon")
    plane = lat_pos // slab
    here = lax.rem(lat_pos, slab) * lon_count + lon_pos
    lower = plane < planes // 2
    home = plane == lon_pos
    last = planes - 1
    late_core = lax.rem(lon_pos, 2) == 0
    partner = lon_pos + 1 - 2 * lax.rem(lon_pos, 2)

    def order(n):
        block, i = n // slab, lax.rem(n, slab)
        early = jnp.where(lower, last - 1 - block, block)
        return jnp.where(block < last, early, last) * slab + lax.rem(lat_pos + i, slab)

    levels_in_order = [order(n) for n in range(levels)]

    barrier = pltpu.get_barrier_semaphore()
    to_late = (plane == last).astype(jnp.int32)

    for i in range(slab):
        for j in range(lon_count // 2):
            lat, lon = lon_pos * slab + i, 2 * j + 1 - to_late

            @pl.when(jnp.logical_not(jnp.logical_and(lat == lat_pos, lon == lon_pos)))
            def _(lat=lat, lon=lon):
                pl.semaphore_signal(barrier, inc=1, device_id=(lat, lon), device_id_type=MESH)

    for step in range(1, lon_count):
        pl.semaphore_signal(
            barrier, inc=1, device_id=(lat_pos, lax.rem(lon_pos + step, lon_count)), device_id_type=MESH
        )

    smalls = [
        pltpu.make_async_copy(src, dst, in_sem.at[n])
        for n, (src, dst) in enumerate([
            (mask_hbm, mask), (scale_table_hbm, scale_table), (offset_table_hbm, offset_table),
            (scale_index_hbm, scale_index), (offset_index_hbm, offset_index),
        ])
    ]
    loads = [
        pltpu.make_async_copy(x_hbm.at[:, levels_in_order[n]], xs[n], x_sem.at[n]) for n in range(levels)
    ]
    for copy in smalls:
        copy.start()
    for copy in loads:
        copy.start()
    for copy in smalls:
        copy.wait()

    seen = []
    total = jnp.int32(0)
    for r in range(rows):
        total = total + mask[lon_pos, lat_pos * rows + r]
        seen.append(total)
    picks = []
    for k in range(slots):
        slot = jnp.minimum(k, total - 1)
        pick = jnp.int32(0)
        for r in range(rows - 1):
            pick = pick + (seen[r] <= slot).astype(jnp.int32)
        picks.append(pick)

    which = lax.broadcasted_iota(jnp.int32, (fields, STRIP), 0)
    scales = jnp.zeros((fields, STRIP), jnp.float32)
    offsets = jnp.zeros((fields, STRIP), jnp.float32)
    for f in range(fields):
        scales = jnp.where(which == f, scale_table[scale_index[f]], scales)
        offsets = jnp.where(which == f, offset_table[offset_index[f]], offsets)

    for n in range(levels):
        loads[n].wait()
        lines = xs[n].reshape(fields * rows, STRIP)
        high = None
        for k in range(slots):
            strip = lines[pl.ds(picks[k], fields, stride=rows), :]
            packed = (strip - offsets) * scales
            send[n, k] = packed
            high = packed if k == 0 else jnp.maximum(high, packed)
            low = -packed if k == 0 else jnp.maximum(low, -packed)
        level = levels_in_order[n]
        part[pl.ds(pl.multiple_of(level * fields, fields), fields), :] = high
        part[pl.ds(pl.multiple_of((levels + level) * fields, fields), fields), :] = low

    for j in range(mine.shape[0]):
        tile = part[j * STRIP:(j + 1) * STRIP, :].T
        mine[j] = jnp.max(tile, axis=0, keepdims=True)

    self_late = jnp.logical_and(home, plane == last)
    count_late = slab - self_late.astype(jnp.int32)
    self_early = jnp.logical_and(home, plane != last)
    count_early = levels - slab - self_early.astype(jnp.int32)
    pl.semaphore_wait(barrier, jnp.where(late_core, count_late, count_early) + lon_count - 1)
    pl.semaphore_signal(token, inc=1, device_id=(lat_pos, partner), device_id_type=MESH)

    def is_self(level):
        return jnp.logical_and(level == lat_pos, home)

    def tell(n):
        return pltpu.make_async_remote_copy(
            src_ref=mine,
            dst_ref=first_stats.at[here],
            send_sem=stat_send.at[n],
            recv_sem=stat_recv.at[here],
            device_id=(order(n), plane),
            device_id_type=MESH,
        )

    def remote(n):
        return pltpu.make_async_remote_copy(
            src_ref=send.at[n],
            dst_ref=recv.at[here],
            send_sem=send_sem.at[n],
            recv_sem=recv_sem.at[here],
            device_id=(order(n), plane),
            device_id_type=MESH,
        )

    def when_remote(n, body):
        pl.when(jnp.logical_not(is_self(order(n))))(body)

    def post(first, end):
        loop(first, end, lambda n: when_remote(n, lambda: tell(n).start()))
        loop(first, end, lambda n: when_remote(n, lambda: remote(n).start()))

    @pl.when(late_core)
    def _():
        pl.semaphore_wait(token, 1)
        loop(0, levels, lambda n: when_remote(n, lambda: tell(n).start()))
        shift = jnp.where(lower, levels - slab, 0)
        loop(shift, levels, lambda n: when_remote(n, lambda: remote(n).start()))
        loop(0, shift, lambda n: when_remote(n, lambda: remote(n).start()))

    @pl.when(jnp.logical_not(late_core))
    def _():
        post(0, levels - slab)
        pl.semaphore_wait(token, 1)
        post(levels - slab, levels)

    @pl.when(home)
    def _():
        first_stats[here] = mine[...]
        block = jnp.where(jnp.logical_and(lower, plane < last), last - 1 - plane, plane)
        recv[here] = send[block * slab]

    def not_me(source, body):
        pl.when(jnp.logical_not(jnp.logical_and(home, source == here)))(body)

    loop(0, sources, lambda source: not_me(source, lambda: pltpu.make_async_copy(
        first_stats.at[source], first_stats.at[source], stat_recv.at[source]).wait()))
    last_stats[lon_pos] = jnp.max(first_stats[...], axis=0)

    def share(step):
        return pltpu.make_async_remote_copy(
            src_ref=last_stats.at[lon_pos],
            dst_ref=last_stats.at[lon_pos],
            send_sem=last_send.at[step],
            recv_sem=last_recv.at[step],
            device_id=(lat_pos, lax.rem(lon_pos + step, lon_count)),
            device_id_type=MESH,
        )

    loop(1, lon_count, lambda n: share(n).start())

    per_field = (slab * rows) * lon_count

    for b in range(lon_count):
        for i in range(slab):
            source = i * lon_count + b
            not_me(source, lambda source=source: pltpu.make_async_copy(
                recv.at[source], recv.at[source], recv_sem.at[source]).wait())
            stage[source] = recv[source]
            rank = jnp.int32(0)
            for r in range(rows):
                live = mask[b, (lon_pos * slab + i) * rows + r]
                strip = stage[source, jnp.minimum(rank, slots - 1)]
                strip = jnp.where(live > 0, strip, 0.0)
                line = i * rows + r
                start = (line // 8 * lon_count + b) * 8 + line % 8
                out[pl.ds(start, fields, stride=per_field), :] = strip
                rank = rank + live

    loop(1, lon_count, lambda n: share(n).wait())
    for end in range(2):
        first = (end * levels + lat_pos) * fields
        best = jnp.max(last_stats[:, first // STRIP], axis=0)
        best = jnp.broadcast_to(best, (8, STRIP))
        own = pltpu.roll(best, lax.rem(STRIP - lax.rem(first, STRIP), STRIP), 1)
        own = own[:1, :fields]
        rng[end] = own if end == 0 else -own

    loop(0, levels, lambda n: when_remote(n, lambda: remote(n).wait_send()))
    loop(0, levels, lambda n: when_remote(n, lambda: tell(n).wait_send()))


def store(history, record_range, history_out, record_range_out, sem):
    copies = [
        pltpu.make_async_copy(history, history_out, sem.at[0]),
        pltpu.make_async_copy(record_range, record_range_out, sem.at[1]),
    ]
    for copy in copies:
        copy.start()
    for copy in copies:
        copy.wait()


def per_device(fields, ocean_mask, scale_table, offset_table, scale_index, offset_index):
    nfield, levels, rows, cells = fields.shape
    lat_count = lax.axis_size("lat")
    lon_count = lax.axis_size("lon")
    slab = lat_count // lon_count
    slots = min(MAX_LIVE, rows)
    sources = slab * lon_count
    out_rows = nfield * slab * rows * lon_count
    stat_rows = 2 * levels * nfield // STRIP
    hbm = pl.BlockSpec(memory_space=pltpu.HBM)
    vmem = pl.BlockSpec(memory_space=pltpu.VMEM)
    history, record_range = pl.pallas_call(
        functools.partial(exchange, (nfield, levels, rows, lat_count, lon_count)),
        out_shape=(
            pltpu.VMEM((out_rows, STRIP), jnp.float32),
            pltpu.VMEM((2, 1, nfield), jnp.float32),
        ),
        in_specs=[hbm] * 6,
        out_specs=(vmem, vmem),
        scratch_shapes=[pltpu.VMEM((nfield, rows, STRIP), jnp.float32)] * levels + [
            pltpu.SMEM((lon_count, lat_count * rows), jnp.int32),
            pltpu.SMEM(scale_table.shape, jnp.float32),
            pltpu.SMEM(offset_table.shape, jnp.float32),
            pltpu.SMEM(scale_index.shape, jnp.int32),
            pltpu.SMEM(offset_index.shape, jnp.int32),
            pltpu.VMEM((levels, slots, nfield, STRIP), jnp.float32),
            pltpu.VMEM((sources, slots, nfield, STRIP), jnp.float32),
            pltpu.VMEM((sources, slots, nfield, STRIP), jnp.float32),
            pltpu.VMEM((2 * levels * nfield, STRIP), jnp.float32),
            pltpu.VMEM((stat_rows, 1, STRIP), jnp.float32),
            pltpu.VMEM((sources, stat_rows, 1, STRIP), jnp.float32),
            pltpu.VMEM((lon_count, stat_rows, 1, STRIP), jnp.float32),
            pltpu.SemaphoreType.DMA((levels,)),
            pltpu.SemaphoreType.DMA((5,)),
            pltpu.SemaphoreType.DMA((levels,)),
            pltpu.SemaphoreType.DMA((sources,)),
            pltpu.SemaphoreType.DMA((levels,)),
            pltpu.SemaphoreType.DMA((sources,)),
            pltpu.SemaphoreType.DMA((lon_count,)),
            pltpu.SemaphoreType.DMA((lon_count,)),
            pltpu.SemaphoreType.REGULAR,
        ],
        compiler_params=pltpu.CompilerParams(
            collective_id=0, has_side_effects=True
        ),
    )(ocean_mask.T, scale_table, offset_table, scale_index, offset_index, fields)
    history, record_range = pl.pallas_call(
        store,
        out_shape=(
            jax.ShapeDtypeStruct(history.shape, jnp.float32),
            jax.ShapeDtypeStruct(record_range.shape, jnp.float32),
        ),
        in_specs=[vmem, vmem],
        out_specs=(hbm, hbm),
        scratch_shapes=[pltpu.SemaphoreType.DMA((2,))],
        compiler_params=pltpu.CompilerParams(vmem_limit_bytes=1 << 20),
    )(
        pltpu.with_memory_space_constraint(history, pltpu.VMEM),
        pltpu.with_memory_space_constraint(record_range, pltpu.VMEM),
    )
    history = history.reshape(nfield, slab * rows // 8, lon_count, 8, STRIP)
    history = history.transpose(0, 1, 3, 2, 4)
    return history.reshape(nfield, 1, slab * rows, lon_count * STRIP), record_range.reshape(2, nfield, 1)


def solution(mesh):
    return jax.shard_map(
        per_device,
        mesh=mesh,
        in_specs=(P(None, None, "lat", "lon"), P(), P(), P(), P(), P()),
        out_specs=(P(None, "lat", "lon", None), P(None, None, "lat")),
        check_vma=False,
    )
```

```python
import functools

import jax
import jax.numpy as jnp
from jax import lax
from jax.experimental import pallas as pl
from jax.experimental.pallas import tpu as pltpu
from jax.sharding import PartitionSpec as P

STRIP = 128
MAX_LIVE = 12
MESH = pl.DeviceIdType.MESH


def loop(low, high, body):
    def step(n, carry):
        body(n)
        return carry

    lax.fori_loop(low, high, step, 0)


def unless(condition, body):
    pl.when(jnp.logical_not(condition))(body)


def exchange(
    dims, mask_hbm, scale_table_hbm, offset_table_hbm, scale_index_hbm, offset_index_hbm, x_hbm,
    out, rng,
    mask, scale_table, offset_table, scale_index, offset_index,
    xs, send, recv, stage, part, mine, first_stats, last_stats,
    x_sem, in_sem, send_sem, recv_sem, stat_send, stat_recv, last_send, last_recv, token,
):
    fields, levels, rows, lat_count, lon_count = dims
    slab = lat_count // lon_count
    planes = lat_count // slab
    sources = slab * lon_count
    slots = send.shape[1]
    last = planes - 1
    lat_pos = lax.axis_index("lat")
    lon_pos = lax.axis_index("lon")
    plane = lat_pos // slab
    here = lax.rem(lat_pos, slab) * lon_count + lon_pos
    lower = plane < planes // 2
    home = plane == lon_pos
    partner = lon_pos + 1 - 2 * lax.rem(lon_pos, 2)
    collects = jnp.logical_and(home, lax.rem(lat_pos, slab) == slab - 1)

    def order(n):
        block, i = n // slab, lax.rem(n, slab)
        early = jnp.where(lower, last - 1 - block, block)
        return jnp.where(block < last, early, last) * slab + lax.rem(lat_pos + 1 + i, slab)

    barrier = pltpu.get_barrier_semaphore()

    def signal(sem, lat, lon):
        pl.semaphore_signal(sem, inc=1, device_id=(lat, lon), device_id_type=MESH)

    @pl.when(plane != last)
    def _():
        for i in range(slab):
            for b in range(lon_count):
                lat = lon_pos * slab + i
                itself = jnp.logical_and(lat == lat_pos, b == lon_pos)
                skip = jnp.logical_or(itself, b == lon_pos) if i == slab - 1 else itself
                unless(skip, lambda lat=lat, b=b: signal(barrier, lat, b))

    unless(jnp.logical_or(plane != last, collects), lambda: signal(barrier, lon_pos * slab + slab - 1, lon_pos))
    for step in range(1, lon_count):
        signal(barrier, lat_pos, lax.rem(lon_pos + step, lon_count))
    unless(collects, lambda: signal(barrier, plane * slab + slab - 1, plane))

    smalls = [
        pltpu.make_async_copy(src, dst, in_sem.at[n])
        for n, (src, dst) in enumerate([
            (mask_hbm, mask), (scale_table_hbm, scale_table), (offset_table_hbm, offset_table),
            (scale_index_hbm, scale_index), (offset_index_hbm, offset_index),
        ])
    ]
    for copy in smalls:
        copy.start()
    for n in range(levels):
        pltpu.make_async_copy(x_hbm.at[:, order(n)], xs.at[n], x_sem).start()
    for copy in smalls:
        copy.wait()

    seen = []
    total = jnp.int32(0)
    for r in range(rows):
        total = total + mask[lon_pos, lat_pos * rows + r]
        seen.append(total)
    picks = []
    for k in range(slots):
        pick = jnp.int32(k)
        for r in range(k, rows - 1):
            pick = pick + (seen[r] <= k).astype(jnp.int32)
        picks.append(pick if k == 0 else jnp.where(k < total, pick, picks[-1]))

    which = lax.broadcasted_iota(jnp.int32, (fields, STRIP), 0)
    scales = jnp.zeros((fields, STRIP), jnp.float32)
    offsets = jnp.zeros((fields, STRIP), jnp.float32)
    for f in range(fields):
        scales = jnp.where(which == f, scale_table[scale_index[f]], scales)
        offsets = jnp.where(which == f, offset_table[offset_index[f]], offsets)

    pltpu.make_async_copy(xs, xs, x_sem).wait()
    lines = xs.reshape(levels * fields * rows, STRIP)
    for n in range(levels):
        high = None
        for k in range(slots):
            strip = lines[pl.ds(n * fields * rows + picks[k], fields, stride=rows), :]
            packed = (strip - offsets) * scales
            send[n, k] = packed
            high = packed if k == 0 else jnp.maximum(high, packed)
            low = -packed if k == 0 else jnp.maximum(low, -packed)
        level = order(n)
        part[pl.ds(pl.multiple_of(level * fields, fields), fields), :] = high
        part[pl.ds(pl.multiple_of((levels + level) * fields, fields), fields), :] = low

    for j in range(mine.shape[0]):
        tile = part[j * STRIP:(j + 1) * STRIP, :].T
        mine[j] = jnp.max(tile, axis=0, keepdims=True)

    own_last = jnp.logical_and(home, plane == last).astype(jnp.int32)
    own_early = jnp.logical_and(home, plane != last).astype(jnp.int32)
    calls = jnp.where(collects, slab - own_last + sources - 1, levels - slab - own_early)
    pl.semaphore_wait(barrier, calls + lon_count - 1)

    @pl.when(collects)
    def _():
        def pass_on(step):
            other = lax.rem(here + step, sources)
            signal(token, plane * slab + other // lon_count, lax.rem(other, lon_count))

        loop(1, sources, pass_on)

    @pl.when(jnp.logical_and(plane == partner, lax.rem(lat_pos, slab) == slab - 1))
    def _():
        signal(token, lat_pos, partner)

    def tell(n):
        return pltpu.make_async_remote_copy(
            src_ref=mine,
            dst_ref=first_stats.at[here],
            send_sem=stat_send,
            recv_sem=stat_recv,
            device_id=(order(n), plane),
            device_id_type=MESH,
        )

    def remote(n):
        return pltpu.make_async_remote_copy(
            src_ref=send.at[n],
            dst_ref=recv.at[here],
            send_sem=send_sem,
            recv_sem=recv_sem.at[here],
            device_id=(order(n), plane),
            device_id_type=MESH,
        )

    def unless_self(n, body):
        unless(jnp.logical_and(order(n) == lat_pos, home), body)

    def post(first, end):
        loop(first, end, lambda n: unless_self(n, lambda: tell(n).start()))
        loop(first, end, lambda n: unless_self(n, lambda: remote(n).start()))

    @pl.when(collects)
    def _():
        pl.semaphore_wait(token, 1)

    post(0, levels - slab)

    @pl.when(jnp.logical_not(collects))
    def _():
        pl.semaphore_wait(token, 1)

    post(levels - slab, levels)

    @pl.when(home)
    def _():
        first_stats[here] = mine[...]
        block = jnp.where(jnp.logical_and(lower, plane < last), last - 1 - plane, plane)
        recv[here] = send[block * slab + slab - 1]

    def wait_all(ref, sem):
        count = ref.shape[0]

        @pl.when(home)
        def _():
            some = ref.at[pl.ds(0, count - 1)]
            pltpu.make_async_copy(some, some, sem).wait()

        unless(home, lambda: pltpu.make_async_copy(ref, ref, sem).wait())

    wait_all(first_stats, stat_recv)
    last_stats[lon_pos] = jnp.max(first_stats[...], axis=0)

    def share(step):
        return pltpu.make_async_remote_copy(
            src_ref=last_stats.at[lon_pos],
            dst_ref=last_stats.at[lon_pos],
            send_sem=last_send,
            recv_sem=last_recv,
            device_id=(lat_pos, lax.rem(lon_pos + step, lon_count)),
            device_id_type=MESH,
        )

    loop(1, lon_count, lambda n: share(n).start())

    def finish_range():
        others = last_stats.at[pl.ds(0, lon_count - 1)]
        pltpu.make_async_copy(others, others, last_recv).wait()
        for end in range(2):
            first = (end * levels + lat_pos) * fields
            best = jnp.max(last_stats[:, first // STRIP], axis=0)
            best = jnp.broadcast_to(best, (8, STRIP))
            own = pltpu.roll(best, lax.rem(STRIP - lax.rem(first, STRIP), STRIP), 1)
            own = own[:1, :fields]
            rng[end] = own if end == 0 else -own

    per_field = (slab * rows) * lon_count

    for turn in range(sources):
        b, i = turn // slab, turn % slab
        source = i * lon_count + b
        if turn == sources - 1:
            finish_range()
        unless(jnp.logical_and(home, source == here), lambda source=source: pltpu.make_async_copy(
            recv.at[source], recv.at[source], recv_sem.at[source]).wait())
        stage[source] = recv[source]
        rank = jnp.int32(0)
        for r in range(rows):
            live = mask[b, (lon_pos * slab + i) * rows + r]
            strip = stage[source, jnp.minimum(rank, slots - 1)]
            strip = jnp.where(live > 0, strip, 0.0)
            line = i * rows + r
            start = (line // 8 * lon_count + b) * 8 + line % 8
            out[pl.ds(start, fields, stride=per_field), :] = strip
            rank = rank + live

    others = last_stats.at[pl.ds(0, lon_count - 1)]
    pltpu.make_async_copy(others, others, last_send).wait()
    wait_all(first_stats, stat_send)
    wait_all(send, send_sem)


def store(history, record_range, history_out, record_range_out, sem):
    copies = [
        pltpu.make_async_copy(history, history_out, sem.at[0]),
        pltpu.make_async_copy(record_range, record_range_out, sem.at[1]),
    ]
    for copy in copies:
        copy.start()
    for copy in copies:
        copy.wait()


def per_device(fields, ocean_mask, scale_table, offset_table, scale_index, offset_index):
    nfield, levels, rows, cells = fields.shape
    lat_count = lax.axis_size("lat")
    lon_count = lax.axis_size("lon")
    slab = lat_count // lon_count
    slots = min(MAX_LIVE, rows)
    sources = slab * lon_count
    out_rows = nfield * slab * rows * lon_count
    stat_rows = 2 * levels * nfield // STRIP
    hbm = pl.BlockSpec(memory_space=pltpu.HBM)
    vmem = pl.BlockSpec(memory_space=pltpu.VMEM)
    history, record_range = pl.pallas_call(
        functools.partial(exchange, (nfield, levels, rows, lat_count, lon_count)),
        out_shape=(
            pltpu.VMEM((out_rows, STRIP), jnp.float32),
            pltpu.VMEM((2, 1, nfield), jnp.float32),
        ),
        in_specs=[hbm] * 6,
        out_specs=(vmem, vmem),
        scratch_shapes=[
            pltpu.SMEM((lon_count, lat_count * rows), jnp.int32),
            pltpu.SMEM(scale_table.shape, jnp.float32),
            pltpu.SMEM(offset_table.shape, jnp.float32),
            pltpu.SMEM(scale_index.shape, jnp.int32),
            pltpu.SMEM(offset_index.shape, jnp.int32),
            pltpu.VMEM((levels, nfield, rows, STRIP), jnp.float32),
            pltpu.VMEM((levels, slots, nfield, STRIP), jnp.float32),
            pltpu.VMEM((sources, slots, nfield, STRIP), jnp.float32),
            pltpu.VMEM((sources, slots, nfield, STRIP), jnp.float32),
            pltpu.VMEM((2 * levels * nfield, STRIP), jnp.float32),
            pltpu.VMEM((stat_rows, 1, STRIP), jnp.float32),
            pltpu.VMEM((sources, stat_rows, 1, STRIP), jnp.float32),
            pltpu.VMEM((lon_count, stat_rows, 1, STRIP), jnp.float32),
            pltpu.SemaphoreType.DMA,
            pltpu.SemaphoreType.DMA((5,)),
            pltpu.SemaphoreType.DMA,
            pltpu.SemaphoreType.DMA((sources,)),
            pltpu.SemaphoreType.DMA,
            pltpu.SemaphoreType.DMA,
            pltpu.SemaphoreType.DMA,
            pltpu.SemaphoreType.DMA,
            pltpu.SemaphoreType.REGULAR,
        ],
        compiler_params=pltpu.CompilerParams(
            collective_id=0, has_side_effects=True
        ),
    )(ocean_mask.T, scale_table, offset_table, scale_index, offset_index, fields)
    history, record_range = pl.pallas_call(
        store,
        out_shape=(
            jax.ShapeDtypeStruct(history.shape, jnp.float32),
            jax.ShapeDtypeStruct(record_range.shape, jnp.float32),
        ),
        in_specs=[vmem, vmem],
        out_specs=(hbm, hbm),
        scratch_shapes=[pltpu.SemaphoreType.DMA((2,))],
        compiler_params=pltpu.CompilerParams(vmem_limit_bytes=1 << 20),
    )(
        pltpu.with_memory_space_constraint(history, pltpu.VMEM),
        pltpu.with_memory_space_constraint(record_range, pltpu.VMEM),
    )
    history = history.reshape(nfield, slab * rows // 8, lon_count, 8, STRIP)
    history = history.transpose(0, 1, 3, 2, 4)
    return history.reshape(nfield, 1, slab * rows, lon_count * STRIP), record_range.reshape(2, nfield, 1)


def solution(mesh):
    return jax.shard_map(
        per_device,
        mesh=mesh,
        in_specs=(P(None, None, "lat", "lon"), P(), P(), P(), P(), P()),
        out_specs=(P(None, "lat", "lon", None), P(None, None, "lat")),
        check_vma=False,
    )
```

```python
import functools

import jax
import jax.numpy as jnp
from jax import lax
from jax.experimental import pallas as pl
from jax.experimental.pallas import tpu as pltpu
from jax.sharding import PartitionSpec as P

STRIP = 128
MAX_LIVE = 12
MESH = pl.DeviceIdType.MESH


def loop(low, high, body):
    def step(n, carry):
        body(n)
        return carry

    lax.fori_loop(low, high, step, 0)


def unless(condition, body):
    pl.when(jnp.logical_not(condition))(body)


def exchange(
    dims, mask_hbm, scale_table_hbm, offset_table_hbm, scale_index_hbm, offset_index_hbm, x_hbm,
    out, rng,
    mask, scale_table, offset_table, scale_index, offset_index,
    xs, send, recv, stage, part, mine, first_stats, last_stats, best,
    x_sem, in_sem, send_sem, recv_sem, stat_send, stat_recv, last_send, last_recv, best_send, best_recv,
    token, cross,
):
    fields, levels, rows, lat_count, lon_count = dims
    slab = lat_count // lon_count
    planes = lat_count // slab
    sources = slab * lon_count
    slots = send.shape[1]
    last = planes - 1
    lat_pos = lax.axis_index("lat")
    lon_pos = lax.axis_index("lon")
    plane = lat_pos // slab
    here = lax.rem(lat_pos, slab) * lon_count + lon_pos
    lower = plane < planes // 2
    home = plane == lon_pos
    x_pos = lax.rem(lat_pos, slab)
    partner = lon_pos + 1 - 2 * lax.rem(lon_pos, 2)
    at_end = x_pos == slab - 1
    collects = jnp.logical_and(home, at_end)
    helps = jnp.logical_and(plane == partner, at_end)

    def place(block):
        early = jnp.where(lower, last - 1 - block, block)
        return jnp.where(block < last, early, last)

    def order(n):
        return place(n // slab) * slab + lax.rem(x_pos + lax.rem(n, slab), slab)

    barrier = pltpu.get_barrier_semaphore()

    def signal(sem, lat, lon):
        pl.semaphore_signal(sem, inc=1, device_id=(lat, lon), device_id_type=MESH)

    @pl.when(plane != last)
    def _():
        for b in range(lon_count):
            skip = jnp.logical_and(b == lon_pos, jnp.logical_or(home, at_end))
            unless(skip, lambda b=b: signal(barrier, lon_pos * slab + x_pos, b))

    for step in range(1, slab):
        signal(barrier, plane * slab + lax.rem(x_pos + step, slab), lon_pos)
    unless(jnp.logical_or(plane != last, collects), lambda: signal(barrier, lon_pos * slab + slab - 1, lon_pos))
    unless(collects, lambda: signal(barrier, plane * slab + slab - 1, plane))
    pl.when(collects)(lambda: signal(barrier, lat_pos, partner))

    @pl.when(plane != last)
    def _():
        for step in range(1, planes):
            signal(barrier, lax.rem(plane + step, planes) * slab + x_pos, lon_pos)

    smalls = [
        pltpu.make_async_copy(src, dst, in_sem.at[n])
        for n, (src, dst) in enumerate([
            (mask_hbm, mask), (scale_table_hbm, scale_table), (offset_table_hbm, offset_table),
            (scale_index_hbm, scale_index), (offset_index_hbm, offset_index),
        ])
    ]
    for copy in smalls:
        copy.start()
    for n in range(levels):
        pltpu.make_async_copy(x_hbm.at[:, order(n)], xs.at[n], x_sem).start()
    for copy in smalls:
        copy.wait()

    seen = []
    total = jnp.int32(0)
    for r in range(rows):
        total = total + mask[lon_pos, lat_pos * rows + r]
        seen.append(total)
    picks = []
    for k in range(slots):
        pick = jnp.int32(k)
        for r in range(k, rows - 1):
            pick = pick + (seen[r] <= k).astype(jnp.int32)
        picks.append(pick if k == 0 else jnp.where(k < total, pick, picks[-1]))

    which = lax.broadcasted_iota(jnp.int32, (fields, STRIP), 0)
    scales = jnp.zeros((fields, STRIP), jnp.float32)
    offsets = jnp.zeros((fields, STRIP), jnp.float32)
    for f in range(fields):
        scales = jnp.where(which == f, scale_table[scale_index[f]], scales)
        offsets = jnp.where(which == f, offset_table[offset_index[f]], offsets)

    pltpu.make_async_copy(xs, xs, x_sem).wait()
    lines = xs.reshape(levels * fields * rows, STRIP)
    for n in range(levels):
        high = None
        for k in range(slots):
            strip = lines[pl.ds(n * fields * rows + picks[k], fields, stride=rows), :]
            packed = (strip - offsets) * scales
            send[n, k] = packed
            high = packed if k == 0 else jnp.maximum(high, packed)
            low = -packed if k == 0 else jnp.maximum(low, -packed)
        level = order(n)
        part[pl.ds(pl.multiple_of(level * fields, fields), fields), :] = high
        part[pl.ds(pl.multiple_of((levels + level) * fields, fields), fields), :] = low

    for j in range(mine.shape[0]):
        tile = part[j * STRIP:(j + 1) * STRIP, :].T
        mine[j] = jnp.max(tile, axis=0, keepdims=True)

    inner = (plane != last).astype(jnp.int32)
    own = home.astype(jnp.int32)
    column = planes - 1 - inner
    calls = jnp.where(
        collects, slab - own * (1 - inner) + sources - 1, planes - 1 - own * inner + helps.astype(jnp.int32)
    )
    pl.semaphore_wait(barrier, column + slab - 1 + calls)

    def row_copy(src, dst, send, receive, lat, lon):
        return pltpu.make_async_remote_copy(
            src_ref=src, dst_ref=dst, send_sem=send, recv_sem=receive,
            device_id=(lat, lon), device_id_type=MESH,
        )

    def tell(other):
        return row_copy(
            mine, first_stats.at[plane], stat_send, stat_recv, other * slab + x_pos, lon_pos
        )

    def unless_here(other, body):
        unless(other == plane, body)

    loop(0, last, lambda other: unless_here(other, lambda: tell(other).start()))

    @pl.when(collects)
    def _():
        def pass_on(step):
            other = lax.rem(here + step, sources)
            signal(token, plane * slab + other // lon_count, lax.rem(other, lon_count))

        loop(1, sources, pass_on)
        pl.semaphore_wait(token, 1)

    pl.when(helps)(lambda: signal(token, lat_pos, partner))
    for step in range(1, slab):
        signal(cross, plane * slab + lax.rem(x_pos + step, slab), lon_pos)

    def remote(n):
        return pltpu.make_async_remote_copy(
            src_ref=send.at[n],
            dst_ref=recv.at[here],
            send_sem=send_sem,
            recv_sem=recv_sem.at[here],
            device_id=(order(n), plane),
            device_id_type=MESH,
        )

    def post(block, first, end):
        def start(i):
            n = block * slab + i
            unless(jnp.logical_and(order(n) == lat_pos, home), lambda: remote(n).start())

        loop(first, end, start)

    post(0, 0, 1)
    pl.semaphore_wait(cross, slab - 1)
    post(0, 1, slab)

    def post_block(block):
        post(block, 1, slab)
        post(block, 0, 1)

    loop(1, last, post_block)

    @pl.when(jnp.logical_not(collects))
    def _():
        pl.semaphore_wait(token, 1)

    post_block(last)
    first_stats[plane] = mine[...]

    @pl.when(home)
    def _():
        block = jnp.where(jnp.logical_and(lower, plane < last), last - 1 - plane, plane)
        recv[here] = send[block * slab]

    def wait_rows(ref, count, sem):
        some = ref.at[pl.ds(0, count)]
        pltpu.make_async_copy(some, some, sem).wait()

    def share(step):
        other = lax.rem(here + step, sources)
        return row_copy(
            last_stats.at[here], last_stats.at[here], last_send, last_recv,
            plane * slab + other // lon_count, lax.rem(other, lon_count),
        )

    @pl.when(plane != last)
    def _():
        wait_rows(first_stats, planes - 1, stat_recv)
        last_stats[here] = jnp.max(first_stats[...], axis=0)
        loop(1, sources, lambda step: share(step).start())

    forward = row_copy(best, best, best_send, best_recv, last * slab + x_pos, lon_pos)

    def finish_range():
        @pl.when(plane != last)
        def _():
            wait_rows(last_stats, sources - 1, last_recv)
            best[...] = jnp.max(last_stats[...], axis=0)

        pl.when(plane == last - 1)(forward.start)
        pl.when(plane == last)(lambda: pltpu.make_async_copy(best, best, best_recv).wait())
        for end in range(2):
            first = (end * levels + lat_pos) * fields
            line = jnp.broadcast_to(best[first // STRIP], (8, STRIP))
            line = pltpu.roll(line, lax.rem(STRIP - lax.rem(first, STRIP), STRIP), 1)
            line = line[:1, :fields]
            rng[end] = line if end == 0 else -line

    per_field = (slab * rows) * lon_count
    pairs = lon_count // 2

    for turn in range(sources):
        core, j, i = 1 - turn // (pairs * slab), turn // slab % pairs, slab - 1 - turn % slab
        b = 2 * lax.rem(lon_pos // 2 + j, pairs) + core
        source = i * lon_count + b
        if turn == sources - 1:
            finish_range()
        unless(jnp.logical_and(home, source == here), lambda source=source: pltpu.make_async_copy(
            recv.at[source], recv.at[source], recv_sem.at[source]).wait())
        stage[source] = recv[source]
        rank = jnp.int32(0)
        for r in range(rows):
            live = mask[b, (lon_pos * slab + i) * rows + r]
            strip = stage[source, jnp.minimum(rank, slots - 1)]
            strip = jnp.where(live > 0, strip, 0.0)
            line = i * rows + r
            start = (line // 8 * lon_count + b) * 8 + line % 8
            out[pl.ds(start, fields, stride=per_field), :] = strip
            rank = rank + live

    pl.when(plane == last - 1)(forward.wait_send)

    @pl.when(plane != last)
    def _():
        wait_rows(last_stats, sources - 1, last_send)
        wait_rows(first_stats, last - 1, stat_send)

    pl.when(plane == last)(lambda: wait_rows(first_stats, last, stat_send))
    pl.when(home)(lambda: wait_rows(send, levels - 1, send_sem))
    unless(home, lambda: wait_rows(send, levels, send_sem))


def store(history, record_range, history_out, record_range_out, sem):
    copies = [
        pltpu.make_async_copy(history, history_out, sem.at[0]),
        pltpu.make_async_copy(record_range, record_range_out, sem.at[1]),
    ]
    for copy in copies:
        copy.start()
    for copy in copies:
        copy.wait()


def per_device(fields, ocean_mask, scale_table, offset_table, scale_index, offset_index):
    nfield, levels, rows, cells = fields.shape
    lat_count = lax.axis_size("lat")
    lon_count = lax.axis_size("lon")
    slab = lat_count // lon_count
    slots = min(MAX_LIVE, rows)
    sources = slab * lon_count
    out_rows = nfield * slab * rows * lon_count
    stat_rows = 2 * levels * nfield // STRIP
    hbm = pl.BlockSpec(memory_space=pltpu.HBM)
    vmem = pl.BlockSpec(memory_space=pltpu.VMEM)
    history, record_range = pl.pallas_call(
        functools.partial(exchange, (nfield, levels, rows, lat_count, lon_count)),
        out_shape=(
            pltpu.VMEM((out_rows, STRIP), jnp.float32),
            pltpu.VMEM((2, 1, nfield), jnp.float32),
        ),
        in_specs=[hbm] * 6,
        out_specs=(vmem, vmem),
        scratch_shapes=[
            pltpu.SMEM((lon_count, lat_count * rows), jnp.int32),
            pltpu.SMEM(scale_table.shape, jnp.float32),
            pltpu.SMEM(offset_table.shape, jnp.float32),
            pltpu.SMEM(scale_index.shape, jnp.int32),
            pltpu.SMEM(offset_index.shape, jnp.int32),
            pltpu.VMEM((levels, nfield, rows, STRIP), jnp.float32),
            pltpu.VMEM((levels, slots, nfield, STRIP), jnp.float32),
            pltpu.VMEM((sources, slots, nfield, STRIP), jnp.float32),
            pltpu.VMEM((sources, slots, nfield, STRIP), jnp.float32),
            pltpu.VMEM((2 * levels * nfield, STRIP), jnp.float32),
            pltpu.VMEM((stat_rows, 1, STRIP), jnp.float32),
            pltpu.VMEM((lat_count // slab, stat_rows, 1, STRIP), jnp.float32),
            pltpu.VMEM((sources, stat_rows, 1, STRIP), jnp.float32),
            pltpu.VMEM((stat_rows, 1, STRIP), jnp.float32),
            pltpu.SemaphoreType.DMA,
            pltpu.SemaphoreType.DMA((5,)),
            pltpu.SemaphoreType.DMA,
            pltpu.SemaphoreType.DMA((sources,)),
            pltpu.SemaphoreType.DMA,
            pltpu.SemaphoreType.DMA,
            pltpu.SemaphoreType.DMA,
            pltpu.SemaphoreType.DMA,
            pltpu.SemaphoreType.DMA,
            pltpu.SemaphoreType.DMA,
            pltpu.SemaphoreType.REGULAR,
            pltpu.SemaphoreType.REGULAR,
        ],
        compiler_params=pltpu.CompilerParams(
            collective_id=0, has_side_effects=True
        ),
    )(ocean_mask.T, scale_table, offset_table, scale_index, offset_index, fields)
    history, record_range = pl.pallas_call(
        store,
        out_shape=(
            jax.ShapeDtypeStruct(history.shape, jnp.float32),
            jax.ShapeDtypeStruct(record_range.shape, jnp.float32),
        ),
        in_specs=[vmem, vmem],
        out_specs=(hbm, hbm),
        scratch_shapes=[pltpu.SemaphoreType.DMA((2,))],
        compiler_params=pltpu.CompilerParams(vmem_limit_bytes=1 << 20),
    )(
        pltpu.with_memory_space_constraint(history, pltpu.VMEM),
        pltpu.with_memory_space_constraint(record_range, pltpu.VMEM),
    )
    history = history.reshape(nfield, slab * rows // 8, lon_count, 8, STRIP)
    history = history.transpose(0, 1, 3, 2, 4)
    return history.reshape(nfield, 1, slab * rows, lon_count * STRIP), record_range.reshape(2, nfield, 1)


def solution(mesh):
    return jax.shard_map(
        per_device,
        mesh=mesh,
        in_specs=(P(None, None, "lat", "lon"), P(), P(), P(), P(), P()),
        out_specs=(P(None, "lat", "lon", None), P(None, None, "lat")),
        check_vma=False,
    )
```

```python
import functools

import jax
import jax.numpy as jnp
from jax import lax
from jax.experimental import pallas as pl
from jax.experimental.pallas import tpu as pltpu
from jax.sharding import PartitionSpec as P

STRIP = 128
MAX_LIVE = 12
MESH = pl.DeviceIdType.MESH


def loop(low, high, body):
    def step(n, carry):
        body(n)
        return carry

    lax.fori_loop(low, high, step, 0)


def unless(condition, body):
    pl.when(jnp.logical_not(condition))(body)


def exchange(
    dims, mask_hbm, scale_table_hbm, offset_table_hbm, scale_index_hbm, offset_index_hbm, x_hbm,
    out, rng,
    mask, scale_table, offset_table, scale_index, offset_index,
    xs, send, recv, stage, part, mine, first_stats, last_stats, best,
    x_sem, in_sem, send_sem, recv_sem, stat_send, stat_recv, last_send, last_recv, best_send, best_recv,
    token, cross,
):
    fields, levels, rows, lat_count, lon_count = dims
    slab = lat_count // lon_count
    planes = lat_count // slab
    sources = slab * lon_count
    slots = send.shape[1]
    last = planes - 1
    lat_pos = lax.axis_index("lat")
    lon_pos = lax.axis_index("lon")
    plane = lat_pos // slab
    here = lax.rem(lat_pos, slab) * lon_count + lon_pos
    lower = plane < planes // 2
    home = plane == lon_pos
    x_pos = lax.rem(lat_pos, slab)
    partner = lon_pos + 1 - 2 * lax.rem(lon_pos, 2)
    at_end = x_pos == slab - 1
    collects = jnp.logical_and(home, at_end)
    helps = jnp.logical_and(plane == partner, at_end)

    def place(block):
        early = jnp.where(lower, last - 1 - block, block)
        return jnp.where(block < last, early, last)

    def order(n):
        return place(n // slab) * slab + lax.rem(x_pos + lax.rem(n, slab), slab)

    barrier = pltpu.get_barrier_semaphore()

    def signal(sem, lat, lon):
        pl.semaphore_signal(sem, inc=1, device_id=(lat, lon), device_id_type=MESH)

    @pl.when(plane != last)
    def _():
        for b in range(lon_count):
            skip = jnp.logical_and(b == lon_pos, jnp.logical_or(home, at_end))
            unless(skip, lambda b=b: signal(barrier, lon_pos * slab + x_pos, b))

    smalls = [
        pltpu.make_async_copy(src, dst, in_sem.at[n])
        for n, (src, dst) in enumerate([
            (mask_hbm, mask), (scale_table_hbm, scale_table), (offset_table_hbm, offset_table),
            (scale_index_hbm, scale_index), (offset_index_hbm, offset_index),
        ])
    ]
    for copy in smalls:
        copy.start()
    for n in range(levels):
        pltpu.make_async_copy(x_hbm.at[:, order(n)], xs.at[n], x_sem).start()
    for step in range(1, slab):
        signal(barrier, plane * slab + lax.rem(x_pos + step, slab), lon_pos)
    unless(jnp.logical_or(plane != last, collects), lambda: signal(barrier, lon_pos * slab + slab - 1, lon_pos))
    unless(collects, lambda: signal(barrier, plane * slab + slab - 1, plane))
    pl.when(collects)(lambda: signal(barrier, lat_pos, partner))

    @pl.when(plane != last)
    def _():
        for step in range(1, planes):
            signal(barrier, lax.rem(plane + step, planes) * slab + x_pos, lon_pos)

    for copy in smalls:
        copy.wait()

    seen = []
    total = jnp.int32(0)
    for r in range(rows):
        total = total + mask[lon_pos, lat_pos * rows + r]
        seen.append(total)
    picks = []
    for k in range(slots):
        pick = jnp.int32(k)
        for r in range(k, rows - 1):
            pick = pick + (seen[r] <= k).astype(jnp.int32)
        picks.append(pick if k == 0 else jnp.where(k < total, pick, picks[-1]))

    which = lax.broadcasted_iota(jnp.int32, (fields, STRIP), 0)
    scales = jnp.zeros((fields, STRIP), jnp.float32)
    offsets = jnp.zeros((fields, STRIP), jnp.float32)
    for f in range(fields):
        scales = jnp.where(which == f, scale_table[scale_index[f]], scales)
        offsets = jnp.where(which == f, offset_table[offset_index[f]], offsets)

    pltpu.make_async_copy(xs, xs, x_sem).wait()
    lines = xs.reshape(levels * fields * rows, STRIP)
    for n in range(levels):
        high = None
        for k in range(slots):
            strip = lines[pl.ds(n * fields * rows + picks[k], fields, stride=rows), :]
            packed = (strip - offsets) * scales
            send[n, k] = packed
            high = packed if k == 0 else jnp.maximum(high, packed)
            low = -packed if k == 0 else jnp.maximum(low, -packed)
        level = order(n)
        part[pl.ds(pl.multiple_of(level * fields, fields), fields), :] = high
        part[pl.ds(pl.multiple_of((levels + level) * fields, fields), fields), :] = low

    for j in range(mine.shape[0]):
        tile = part[j * STRIP:(j + 1) * STRIP, :].T
        mine[j] = jnp.max(tile, axis=0, keepdims=True)

    inner = (plane != last).astype(jnp.int32)
    own = home.astype(jnp.int32)
    column = planes - 1 - inner
    calls = jnp.where(
        collects, slab - own * (1 - inner) + sources - 1, planes - 1 - own * inner + helps.astype(jnp.int32)
    )
    pl.semaphore_wait(barrier, column + slab - 1 + calls)

    def row_copy(src, dst, send, receive, lat, lon):
        return pltpu.make_async_remote_copy(
            src_ref=src, dst_ref=dst, send_sem=send, recv_sem=receive,
            device_id=(lat, lon), device_id_type=MESH,
        )

    def tell(other):
        return row_copy(
            mine, first_stats.at[plane], stat_send, stat_recv, other * slab + x_pos, lon_pos
        )

    def unless_here(other, body):
        unless(other == plane, body)

    @pl.when(collects)
    def _():
        def pass_on(step):
            other = lax.rem(here + step, sources)
            signal(token, plane * slab + other // lon_count, lax.rem(other, lon_count))

        loop(1, sources, pass_on)
        pl.semaphore_wait(token, 1)

    pl.when(helps)(lambda: signal(token, lat_pos, partner))
    for step in range(1, slab):
        signal(cross, plane * slab + lax.rem(x_pos + step, slab), lon_pos)

    loop(0, last, lambda other: unless_here(other, lambda: tell(other).start()))

    def remote(n):
        return pltpu.make_async_remote_copy(
            src_ref=send.at[n],
            dst_ref=recv.at[here],
            send_sem=send_sem,
            recv_sem=recv_sem.at[here],
            device_id=(order(n), plane),
            device_id_type=MESH,
        )

    def post(block, first, end):
        def start(i):
            n = block * slab + i
            unless(jnp.logical_and(order(n) == lat_pos, home), lambda: remote(n).start())

        loop(first, end, start)

    post(0, 0, 1)
    pl.semaphore_wait(cross, slab - 1)
    post(0, 1, slab)

    def post_block(block):
        post(block, 1, slab)
        post(block, 0, 1)

    loop(1, last, post_block)

    @pl.when(jnp.logical_not(collects))
    def _():
        pl.semaphore_wait(token, 1)

    post_block(last)
    first_stats[plane] = mine[...]

    @pl.when(home)
    def _():
        block = jnp.where(jnp.logical_and(lower, plane < last), last - 1 - plane, plane)
        recv[here] = send[block * slab]

    def wait_rows(ref, count, sem):
        some = ref.at[pl.ds(0, count)]
        pltpu.make_async_copy(some, some, sem).wait()

    def share(step):
        other = lax.rem(here + step, sources)
        return row_copy(
            last_stats.at[here], last_stats.at[here], last_send, last_recv,
            plane * slab + other // lon_count, lax.rem(other, lon_count),
        )

    @pl.when(plane != last)
    def _():
        wait_rows(first_stats, planes - 1, stat_recv)
        last_stats[here] = jnp.max(first_stats[...], axis=0)
        loop(1, sources, lambda step: share(step).start())

    forward = row_copy(best, best, best_send, best_recv, last * slab + x_pos, lon_pos)

    def finish_range():
        @pl.when(plane != last)
        def _():
            wait_rows(last_stats, sources - 1, last_recv)
            best[...] = jnp.max(last_stats[...], axis=0)

        pl.when(plane == last - 1)(forward.start)
        pl.when(plane == last)(lambda: pltpu.make_async_copy(best, best, best_recv).wait())
        for end in range(2):
            first = (end * levels + lat_pos) * fields
            line = jnp.broadcast_to(best[first // STRIP], (8, STRIP))
            line = pltpu.roll(line, lax.rem(STRIP - lax.rem(first, STRIP), STRIP), 1)
            line = line[:1, :fields]
            rng[end] = line if end == 0 else -line

    per_field = out.shape[0] // fields
    pairs = lon_count // 2
    crossed = lower == (lon_pos >= planes // 2)

    def drain():
        pl.when(plane == last - 1)(forward.wait_send)

        @pl.when(plane != last)
        def _():
            wait_rows(last_stats, sources - 1, last_send)
            wait_rows(first_stats, last - 1, stat_send)

        pl.when(plane == last)(lambda: wait_rows(first_stats, last, stat_send))
        pl.when(home)(lambda: wait_rows(send, levels - 1, send_sem))
        unless(home, lambda: wait_rows(send, levels, send_sem))

    for turn in range(sources):
        core, i, j = 1 - turn // (pairs * slab), turn // pairs % slab, turn % pairs
        b = 2 * lax.rem(lon_pos // 2 + j, pairs) + core
        source = i * lon_count + b
        if turn == 0:
            pl.when(plane == last - 1)(finish_range)
        if turn == sources // 2:
            pl.when(jnp.logical_and(crossed, plane != last - 1))(finish_range)
        if turn == sources - 1:
            pl.when(jnp.logical_not(jnp.logical_or(crossed, plane == last - 1)))(finish_range)
            drain()
        unless(jnp.logical_and(home, source == here), lambda source=source: pltpu.make_async_copy(
            recv.at[source], recv.at[source], recv_sem.at[source]).wait())
        stage[source] = recv[source]
        rank = jnp.int32(0)
        for r in range(rows):
            live = mask[b, (lon_pos * slab + i) * rows + r]
            strip = stage[source, jnp.minimum(rank, slots - 1)]
            strip = jnp.where(live > 0, strip, 0.0)
            line = i * rows + r
            start = (line // 8 * lon_count + b) * 8 + line % 8
            out[pl.ds(start, fields, stride=per_field), :] = strip
            rank = rank + live


def store(history, record_range, history_out, record_range_out, sem):
    copies = [
        pltpu.make_async_copy(history.at[:, pl.ds(0, history_out.shape[1])], history_out, sem.at[0]),
        pltpu.make_async_copy(record_range, record_range_out, sem.at[1]),
    ]
    for copy in copies:
        copy.start()
    for copy in copies:
        copy.wait()


def per_device(fields, ocean_mask, scale_table, offset_table, scale_index, offset_index):
    nfield, levels, rows, cells = fields.shape
    lat_count = lax.axis_size("lat")
    lon_count = lax.axis_size("lon")
    slab = lat_count // lon_count
    slots = min(MAX_LIVE, rows)
    sources = slab * lon_count
    per_field = slab * rows * lon_count
    stat_rows = 2 * levels * nfield // STRIP
    hbm = pl.BlockSpec(memory_space=pltpu.HBM)
    vmem = pl.BlockSpec(memory_space=pltpu.VMEM)
    history, record_range = pl.pallas_call(
        functools.partial(exchange, (nfield, levels, rows, lat_count, lon_count)),
        out_shape=(
            pltpu.VMEM((nfield * (per_field + 8), STRIP), jnp.float32),
            pltpu.VMEM((2, 1, nfield), jnp.float32),
        ),
        in_specs=[hbm] * 6,
        out_specs=(vmem, vmem),
        scratch_shapes=[
            pltpu.SMEM((lon_count, lat_count * rows), jnp.int32),
            pltpu.SMEM(scale_table.shape, jnp.float32),
            pltpu.SMEM(offset_table.shape, jnp.float32),
            pltpu.SMEM(scale_index.shape, jnp.int32),
            pltpu.SMEM(offset_index.shape, jnp.int32),
            pltpu.VMEM((levels, nfield, rows, STRIP), jnp.float32),
            pltpu.VMEM((levels, slots, nfield, STRIP), jnp.float32),
            pltpu.VMEM((sources, slots, nfield, STRIP), jnp.float32),
            pltpu.VMEM((sources, slots, nfield, STRIP), jnp.float32),
            pltpu.VMEM((2 * levels * nfield, STRIP), jnp.float32),
            pltpu.VMEM((stat_rows, 1, STRIP), jnp.float32),
            pltpu.VMEM((lat_count // slab, stat_rows, 1, STRIP), jnp.float32),
            pltpu.VMEM((sources, stat_rows, 1, STRIP), jnp.float32),
            pltpu.VMEM((stat_rows, 1, STRIP), jnp.float32),
            pltpu.SemaphoreType.DMA,
            pltpu.SemaphoreType.DMA((5,)),
            pltpu.SemaphoreType.DMA,
            pltpu.SemaphoreType.DMA((sources,)),
            pltpu.SemaphoreType.DMA,
            pltpu.SemaphoreType.DMA,
            pltpu.SemaphoreType.DMA,
            pltpu.SemaphoreType.DMA,
            pltpu.SemaphoreType.DMA,
            pltpu.SemaphoreType.DMA,
            pltpu.SemaphoreType.REGULAR,
            pltpu.SemaphoreType.REGULAR,
        ],
        compiler_params=pltpu.CompilerParams(
            collective_id=0, has_side_effects=True
        ),
    )(ocean_mask.T, scale_table, offset_table, scale_index, offset_index, fields)
    history, record_range = pl.pallas_call(
        store,
        out_shape=(
            jax.ShapeDtypeStruct((nfield, per_field, STRIP), jnp.float32),
            jax.ShapeDtypeStruct(record_range.shape, jnp.float32),
        ),
        in_specs=[vmem, vmem],
        out_specs=(hbm, hbm),
        scratch_shapes=[pltpu.SemaphoreType.DMA((2,))],
        compiler_params=pltpu.CompilerParams(vmem_limit_bytes=1 << 20),
    )(
        pltpu.with_memory_space_constraint(history.reshape(nfield, per_field + 8, STRIP), pltpu.VMEM),
        pltpu.with_memory_space_constraint(record_range, pltpu.VMEM),
    )
    history = history.reshape(nfield, slab * rows // 8, lon_count, 8, STRIP)
    history = history.transpose(0, 1, 3, 2, 4)
    return history.reshape(nfield, 1, slab * rows, lon_count * STRIP), record_range.reshape(2, nfield, 1)


def solution(mesh):
    return jax.shard_map(
        per_device,
        mesh=mesh,
        in_specs=(P(None, None, "lat", "lon"), P(), P(), P(), P(), P()),
        out_specs=(P(None, "lat", "lon", None), P(None, None, "lat")),
        check_vma=False,
    )
```

```python
import functools

import jax
import jax.numpy as jnp
from jax import lax
from jax.experimental import pallas as pl
from jax.experimental.pallas import tpu as pltpu
from jax.sharding import PartitionSpec as P

STRIP = 128
MAX_LIVE = 12
MESH = pl.DeviceIdType.MESH


def loop(low, high, body):
    def step(n, carry):
        body(n)
        return carry

    lax.fori_loop(low, high, step, 0)


def unless(condition, body):
    pl.when(jnp.logical_not(condition))(body)


def exchange(
    dims, mask_hbm, scale_table_hbm, offset_table_hbm, scale_index_hbm, offset_index_hbm, x_hbm,
    out, rng,
    mask, scale_table, offset_table, scale_index, offset_index, after,
    xs, send, recv, stage, part, mine, first_stats, last_stats, best,
    x_sem, in_sem, send_sem, recv_sem, stat_send, stat_recv, last_send, last_recv, best_send, best_recv,
    token, cross,
):
    fields, levels, rows, lat_count, lon_count = dims
    slab = lat_count // lon_count
    planes = lat_count // slab
    sources = slab * lon_count
    slots = send.shape[1]
    last = planes - 1
    lat_pos = lax.axis_index("lat")
    lon_pos = lax.axis_index("lon")
    plane = lat_pos // slab
    here = lax.rem(lat_pos, slab) * lon_count + lon_pos
    lower = plane < planes // 2
    home = plane == lon_pos
    x_pos = lax.rem(lat_pos, slab)
    partner = lon_pos + 1 - 2 * lax.rem(lon_pos, 2)
    at_end = x_pos == slab - 1
    collects = jnp.logical_and(home, at_end)
    helps = jnp.logical_and(plane == partner, at_end)

    def place(block):
        early = jnp.where(lower, last - 1 - block, block)
        return jnp.where(block < last, early, last)

    def order(n):
        return place(n // slab) * slab + lax.rem(x_pos + lax.rem(n, slab), slab)

    barrier = pltpu.get_barrier_semaphore()

    def signal(sem, lat, lon):
        pl.semaphore_signal(sem, inc=1, device_id=(lat, lon), device_id_type=MESH)

    @pl.when(plane != last)
    def _():
        for b in range(lon_count):
            skip = jnp.logical_and(b == lon_pos, jnp.logical_or(home, at_end))
            unless(skip, lambda b=b: signal(barrier, lon_pos * slab + x_pos, b))

    smalls = [
        pltpu.make_async_copy(src, dst, in_sem.at[n])
        for n, (src, dst) in enumerate([
            (mask_hbm, mask), (scale_table_hbm, scale_table), (offset_table_hbm, offset_table),
            (scale_index_hbm, scale_index), (offset_index_hbm, offset_index),
        ])
    ]
    for copy in smalls:
        copy.start()
    for f in range(fields):
        pltpu.make_async_copy(x_hbm.at[f], xs.at[:, :, f], x_sem).start()
    for step in range(1, slab):
        signal(barrier, plane * slab + lax.rem(x_pos + step, slab), lon_pos)
    unless(jnp.logical_or(plane != last, collects), lambda: signal(barrier, lon_pos * slab + slab - 1, lon_pos))
    unless(collects, lambda: signal(barrier, plane * slab + slab - 1, plane))
    pl.when(collects)(lambda: signal(barrier, lat_pos, partner))

    @pl.when(plane != last)
    def _():
        for step in range(1, planes):
            signal(barrier, lax.rem(plane + step, planes) * slab + x_pos, lon_pos)

    for copy in smalls:
        copy.wait()

    following = first = jnp.int32(0)
    for r in reversed(range(rows)):
        first = jnp.where(mask[lon_pos, lat_pos * rows + r] > 0, r, first)
    following = first
    after[rows] = first
    for r in reversed(range(1, rows)):
        following = jnp.where(mask[lon_pos, lat_pos * rows + r] > 0, r, following)
        after[r] = following
    picks = [first]
    for k in range(1, slots):
        picks.append(after[picks[-1] + 1])

    which = lax.broadcasted_iota(jnp.int32, (fields, STRIP), 0)
    scales = jnp.zeros((fields, STRIP), jnp.float32)
    offsets = jnp.zeros((fields, STRIP), jnp.float32)
    for f in range(fields):
        scales = jnp.where(which == f, scale_table[scale_index[f]], scales)
        offsets = jnp.where(which == f, offset_table[offset_index[f]], offsets)

    pltpu.make_async_copy(xs, xs, x_sem).wait()
    for n in range(levels):
        level = order(n)
        high = low = None
        for k in range(slots):
            packed = (xs[level, picks[k]] - offsets) * scales
            send[n, k] = packed
            high = packed if k == 0 else jnp.maximum(high, packed)
            low = packed if k == 0 else jnp.minimum(low, packed)
        part[pl.ds(pl.multiple_of(level * fields, fields), fields), :] = high
        part[pl.ds(pl.multiple_of((levels + level) * fields, fields), fields), :] = -low

    for j in range(mine.shape[0]):
        tile = part[j * STRIP:(j + 1) * STRIP, :].T
        mine[j] = jnp.max(tile, axis=0, keepdims=True)

    inner = (plane != last).astype(jnp.int32)
    own = home.astype(jnp.int32)
    column = planes - 1 - inner
    calls = jnp.where(
        collects, slab - own * (1 - inner) + sources - 1, planes - 1 - own * inner + helps.astype(jnp.int32)
    )
    pl.semaphore_wait(barrier, column + slab - 1 + calls)

    def row_copy(src, dst, send, receive, lat, lon):
        return pltpu.make_async_remote_copy(
            src_ref=src, dst_ref=dst, send_sem=send, recv_sem=receive,
            device_id=(lat, lon), device_id_type=MESH,
        )

    def tell(other):
        return row_copy(
            mine, first_stats.at[plane], stat_send, stat_recv, other * slab + x_pos, lon_pos
        )

    def unless_here(other, body):
        unless(other == plane, body)

    @pl.when(collects)
    def _():
        def pass_on(step):
            other = lax.rem(here + step, sources)
            signal(token, plane * slab + other // lon_count, lax.rem(other, lon_count))

        loop(1, sources, pass_on)
        pl.semaphore_wait(token, 1)

    pl.when(helps)(lambda: signal(token, lat_pos, partner))
    for step in range(1, slab):
        signal(cross, plane * slab + lax.rem(x_pos + step, slab), lon_pos)

    loop(0, last, lambda other: unless_here(other, lambda: tell(other).start()))

    def remote(n):
        return pltpu.make_async_remote_copy(
            src_ref=send.at[n],
            dst_ref=recv.at[here],
            send_sem=send_sem,
            recv_sem=recv_sem.at[here],
            device_id=(order(n), plane),
            device_id_type=MESH,
        )

    def post(block, first, end):
        def start(i):
            n = block * slab + i
            unless(jnp.logical_and(order(n) == lat_pos, home), lambda: remote(n).start())

        loop(first, end, start)

    post(0, 0, 1)
    pl.semaphore_wait(cross, slab - 1)
    post(0, 1, slab)

    def post_block(block):
        post(block, 1, slab)
        post(block, 0, 1)

    loop(1, last, post_block)

    @pl.when(jnp.logical_not(collects))
    def _():
        pl.semaphore_wait(token, 1)

    post_block(last)
    first_stats[plane] = mine[...]

    @pl.when(home)
    def _():
        block = jnp.where(jnp.logical_and(lower, plane < last), last - 1 - plane, plane)
        recv[here] = send[block * slab]

    def wait_rows(ref, count, sem):
        some = ref.at[pl.ds(0, count)]
        pltpu.make_async_copy(some, some, sem).wait()

    def share(step):
        other = lax.rem(here + step, sources)
        return row_copy(
            last_stats.at[here], last_stats.at[here], last_send, last_recv,
            plane * slab + other // lon_count, lax.rem(other, lon_count),
        )

    @pl.when(plane != last)
    def _():
        wait_rows(first_stats, planes - 1, stat_recv)
        last_stats[here] = jnp.max(first_stats[...], axis=0)
        loop(1, sources, lambda step: share(step).start())

    forward = row_copy(best, best, best_send, best_recv, last * slab + x_pos, lon_pos)

    def finish_range():
        @pl.when(plane != last)
        def _():
            wait_rows(last_stats, sources - 1, last_recv)
            best[...] = jnp.max(last_stats[...], axis=0)

        pl.when(plane == last - 1)(forward.start)
        pl.when(plane == last)(lambda: pltpu.make_async_copy(best, best, best_recv).wait())
        for end in range(2):
            first = (end * levels + lat_pos) * fields
            line = jnp.broadcast_to(best[first // STRIP], (8, STRIP))
            line = pltpu.roll(line, lax.rem(STRIP - lax.rem(first, STRIP), STRIP), 1)
            line = line[:1, :fields]
            rng[end] = line if end == 0 else -line

    per_field = out.shape[0] // fields
    pairs = lon_count // 2
    crossed = lower == (lon_pos >= planes // 2)

    def drain():
        pl.when(plane == last - 1)(forward.wait_send)

        @pl.when(plane != last)
        def _():
            wait_rows(last_stats, sources - 1, last_send)
            wait_rows(first_stats, last - 1, stat_send)

        pl.when(plane == last)(lambda: wait_rows(first_stats, last, stat_send))
        pl.when(home)(lambda: wait_rows(send, levels - 1, send_sem))
        unless(home, lambda: wait_rows(send, levels, send_sem))

    for turn in range(sources):
        core, i, j = 1 - turn // (pairs * slab), turn // pairs % slab, turn % pairs
        b = 2 * lax.rem(lon_pos // 2 + j, pairs) + core
        source = i * lon_count + b
        if turn == 0:
            pl.when(plane == last - 1)(finish_range)
        if turn == sources // 2:
            pl.when(jnp.logical_and(crossed, plane != last - 1))(finish_range)
        if turn == sources - 1:
            pl.when(jnp.logical_not(jnp.logical_or(crossed, plane == last - 1)))(finish_range)
            drain()
        unless(jnp.logical_and(home, source == here), lambda source=source: pltpu.make_async_copy(
            recv.at[source], recv.at[source], recv_sem.at[source]).wait())
        stage[source] = recv[source]
        rank = jnp.int32(0)
        for r in range(rows):
            live = mask[b, (lon_pos * slab + i) * rows + r]
            strip = stage[source, jnp.minimum(rank, slots - 1)]
            strip = jnp.where(live > 0, strip, 0.0)
            line = i * rows + r
            start = (line // 8 * lon_count + b) * 8 + line % 8
            out[pl.ds(start, fields, stride=per_field), :] = strip
            rank = rank + live


def store(history, record_range, history_out, record_range_out, sem):
    copies = [
        pltpu.make_async_copy(history.at[:, pl.ds(0, history_out.shape[1])], history_out, sem.at[0]),
        pltpu.make_async_copy(record_range, record_range_out, sem.at[1]),
    ]
    for copy in copies:
        copy.start()
    for copy in copies:
        copy.wait()


def per_device(fields, ocean_mask, scale_table, offset_table, scale_index, offset_index):
    nfield, levels, rows, cells = fields.shape
    lat_count = lax.axis_size("lat")
    lon_count = lax.axis_size("lon")
    slab = lat_count // lon_count
    slots = min(MAX_LIVE, rows)
    sources = slab * lon_count
    per_field = slab * rows * lon_count
    stat_rows = 2 * levels * nfield // STRIP
    hbm = pl.BlockSpec(memory_space=pltpu.HBM)
    vmem = pl.BlockSpec(memory_space=pltpu.VMEM)
    history, record_range = pl.pallas_call(
        functools.partial(exchange, (nfield, levels, rows, lat_count, lon_count)),
        out_shape=(
            pltpu.VMEM((nfield * (per_field + 8), STRIP), jnp.float32),
            pltpu.VMEM((2, 1, nfield), jnp.float32),
        ),
        in_specs=[hbm] * 6,
        out_specs=(vmem, vmem),
        scratch_shapes=[
            pltpu.SMEM((lon_count, lat_count * rows), jnp.int32),
            pltpu.SMEM(scale_table.shape, jnp.float32),
            pltpu.SMEM(offset_table.shape, jnp.float32),
            pltpu.SMEM(scale_index.shape, jnp.int32),
            pltpu.SMEM(offset_index.shape, jnp.int32),
            pltpu.SMEM((rows + 1,), jnp.int32),
            pltpu.VMEM((levels, rows, nfield, STRIP), jnp.float32),
            pltpu.VMEM((levels, slots, nfield, STRIP), jnp.float32),
            pltpu.VMEM((sources, slots, nfield, STRIP), jnp.float32),
            pltpu.VMEM((sources, slots, nfield, STRIP), jnp.float32),
            pltpu.VMEM((2 * levels * nfield, STRIP), jnp.float32),
            pltpu.VMEM((stat_rows, 1, STRIP), jnp.float32),
            pltpu.VMEM((lat_count // slab, stat_rows, 1, STRIP), jnp.float32),
            pltpu.VMEM((sources, stat_rows, 1, STRIP), jnp.float32),
            pltpu.VMEM((stat_rows, 1, STRIP), jnp.float32),
            pltpu.SemaphoreType.DMA,
            pltpu.SemaphoreType.DMA((5,)),
            pltpu.SemaphoreType.DMA,
            pltpu.SemaphoreType.DMA((sources,)),
            pltpu.SemaphoreType.DMA,
            pltpu.SemaphoreType.DMA,
            pltpu.SemaphoreType.DMA,
            pltpu.SemaphoreType.DMA,
            pltpu.SemaphoreType.DMA,
            pltpu.SemaphoreType.DMA,
            pltpu.SemaphoreType.REGULAR,
            pltpu.SemaphoreType.REGULAR,
        ],
        compiler_params=pltpu.CompilerParams(
            collective_id=0, has_side_effects=True
        ),
    )(ocean_mask.T, scale_table, offset_table, scale_index, offset_index, fields)
    history, record_range = pl.pallas_call(
        store,
        out_shape=(
            jax.ShapeDtypeStruct((nfield, per_field, STRIP), jnp.float32),
            jax.ShapeDtypeStruct(record_range.shape, jnp.float32),
        ),
        in_specs=[vmem, vmem],
        out_specs=(hbm, hbm),
        scratch_shapes=[pltpu.SemaphoreType.DMA((2,))],
        compiler_params=pltpu.CompilerParams(vmem_limit_bytes=1 << 20),
    )(
        pltpu.with_memory_space_constraint(history.reshape(nfield, per_field + 8, STRIP), pltpu.VMEM),
        pltpu.with_memory_space_constraint(record_range, pltpu.VMEM),
    )
    history = history.reshape(nfield, slab * rows // 8, lon_count, 8, STRIP)
    history = history.transpose(0, 1, 3, 2, 4)
    return history.reshape(nfield, 1, slab * rows, lon_count * STRIP), record_range.reshape(2, nfield, 1)


def solution(mesh):
    return jax.shard_map(
        per_device,
        mesh=mesh,
        in_specs=(P(None, None, "lat", "lon"), P(), P(), P(), P(), P()),
        out_specs=(P(None, "lat", "lon", None), P(None, None, "lat")),
        check_vma=False,
    )
```

```python
import functools

import jax
import jax.numpy as jnp
from jax import lax
from jax.experimental import pallas as pl
from jax.experimental.pallas import tpu as pltpu
from jax.sharding import PartitionSpec as P

STRIP = 128
MAX_LIVE = 12
MESH = pl.DeviceIdType.MESH


def loop(low, high, body):
    def step(n, carry):
        body(n)
        return carry

    lax.fori_loop(low, high, step, 0)


def unless(condition, body):
    pl.when(jnp.logical_not(condition))(body)


def exchange(
    dims, mask_hbm, scale_table_hbm, offset_table_hbm, scale_index_hbm, offset_index_hbm, x_hbm,
    out, rng,
    mask, scale_table, offset_table, scale_index, offset_index, after,
    xs, send, recv, stage, part, mine, first_stats, last_stats, best,
    x_sem, in_sem, sent, recv_sem, stat_recv, last_recv, best_recv,
    token, cross,
):
    fields, levels, rows, lat_count, lon_count = dims
    slab = lat_count // lon_count
    planes = lat_count // slab
    sources = slab * lon_count
    slots = send.shape[1]
    last = planes - 1
    lat_pos = lax.axis_index("lat")
    lon_pos = lax.axis_index("lon")
    plane = lat_pos // slab
    here = lax.rem(lat_pos, slab) * lon_count + lon_pos
    lower = plane < planes // 2
    home = plane == lon_pos
    x_pos = lax.rem(lat_pos, slab)
    partner = lon_pos + 1 - 2 * lax.rem(lon_pos, 2)
    at_end = x_pos == slab - 1
    collects = jnp.logical_and(home, at_end)
    helps = jnp.logical_and(plane == partner, at_end)

    def place(block):
        early = jnp.where(lower, last - 1 - block, block)
        return jnp.where(block < last, early, last)

    def order(n):
        return place(n // slab) * slab + lax.rem(x_pos + lax.rem(n, slab), slab)

    barrier = pltpu.get_barrier_semaphore()

    def signal(sem, lat, lon):
        pl.semaphore_signal(sem, inc=1, device_id=(lat, lon), device_id_type=MESH)

    @pl.when(plane != last)
    def _():
        for b in range(lon_count):
            skip = jnp.logical_and(b == lon_pos, jnp.logical_or(home, at_end))
            unless(skip, lambda b=b: signal(barrier, lon_pos * slab + x_pos, b))

    @pl.when(plane != last)
    def _():
        for step in range(1, planes):
            signal(barrier, lax.rem(plane + step, planes) * slab + x_pos, lon_pos)

    smalls = [
        pltpu.make_async_copy(src, dst, in_sem)
        for n, (src, dst) in enumerate([
            (mask_hbm, mask), (scale_table_hbm, scale_table), (offset_table_hbm, offset_table),
            (scale_index_hbm, scale_index), (offset_index_hbm, offset_index),
        ])
    ]
    for copy in smalls:
        copy.start()
    for f in range(fields):
        pltpu.make_async_copy(x_hbm.at[f], xs.at[:, :, f], x_sem).start()
    for step in range(1, slab):
        signal(barrier, plane * slab + lax.rem(x_pos + step, slab), lon_pos)
    unless(jnp.logical_or(plane != last, collects), lambda: signal(barrier, lon_pos * slab + slab - 1, lon_pos))
    unless(collects, lambda: signal(barrier, plane * slab + slab - 1, plane))
    pl.when(collects)(lambda: signal(barrier, lat_pos, partner))

    for copy in smalls:
        copy.wait()

    following = first = jnp.int32(0)
    for r in reversed(range(rows)):
        first = jnp.where(mask[lon_pos, lat_pos * rows + r] > 0, r, first)
    following = first
    after[rows] = first
    for r in reversed(range(1, rows)):
        following = jnp.where(mask[lon_pos, lat_pos * rows + r] > 0, r, following)
        after[r] = following
    picks = [first]
    for k in range(1, slots):
        picks.append(after[picks[-1] + 1])

    which = lax.broadcasted_iota(jnp.int32, (fields, STRIP), 0)
    scales = jnp.zeros((fields, STRIP), jnp.float32)
    offsets = jnp.zeros((fields, STRIP), jnp.float32)
    for f in range(fields):
        scales = jnp.where(which == f, scale_table[scale_index[f]], scales)
        offsets = jnp.where(which == f, offset_table[offset_index[f]], offsets)

    pltpu.make_async_copy(xs, xs, x_sem).wait()
    for n in range(levels):
        level = order(n)
        high = low = None
        for k in range(slots):
            packed = (xs[level, picks[k]] - offsets) * scales
            send[n, k] = packed
            high = packed if k == 0 else jnp.maximum(high, packed)
            low = packed if k == 0 else jnp.minimum(low, packed)
        part[pl.ds(pl.multiple_of(level * fields, fields), fields), :] = high
        part[pl.ds(pl.multiple_of((levels + level) * fields, fields), fields), :] = -low

    for j in range(mine.shape[0]):
        tile = part[j * STRIP:(j + 1) * STRIP, :].T
        mine[j] = jnp.max(tile, axis=0, keepdims=True)

    inner = (plane != last).astype(jnp.int32)
    own = home.astype(jnp.int32)
    column = planes - 1 - inner
    calls = jnp.where(
        collects, slab - own * (1 - inner) + sources - 1, planes - 1 - own * inner + helps.astype(jnp.int32)
    )
    pl.semaphore_wait(barrier, column + slab - 1 + calls)

    def row_copy(src, dst, send, receive, lat, lon):
        return pltpu.make_async_remote_copy(
            src_ref=src, dst_ref=dst, send_sem=send, recv_sem=receive,
            device_id=(lat, lon), device_id_type=MESH,
        )

    def tell(other):
        return row_copy(
            mine, first_stats.at[plane], sent, stat_recv, other * slab + x_pos, lon_pos
        )

    def unless_here(other, body):
        unless(other == plane, body)

    @pl.when(collects)
    def _():
        def pass_on(step):
            other = lax.rem(here + step, sources)
            signal(token, plane * slab + other // lon_count, lax.rem(other, lon_count))

        loop(1, sources, pass_on)
        pl.semaphore_wait(token, 1)

    pl.when(helps)(lambda: signal(token, lat_pos, partner))
    for step in range(1, slab):
        signal(cross, plane * slab + lax.rem(x_pos + step, slab), lon_pos)

    loop(0, last, lambda other: unless_here(other, lambda: tell(other).start()))

    def remote(n):
        return pltpu.make_async_remote_copy(
            src_ref=send.at[n],
            dst_ref=recv.at[here],
            send_sem=sent,
            recv_sem=recv_sem.at[here],
            device_id=(order(n), plane),
            device_id_type=MESH,
        )

    def post(block, first, end):
        def start(i):
            n = block * slab + i
            unless(jnp.logical_and(order(n) == lat_pos, home), lambda: remote(n).start())

        loop(first, end, start)

    below = jnp.where(lower, last - plane, last)
    post(0, 0, 1)
    loop(below, last, lambda block: post(block, 0, 1))
    pl.semaphore_wait(cross, slab - 1)
    post(0, 1, slab)

    def post_block(block):
        post(block, 1, slab)
        unless(jnp.logical_and(block >= below, block < last), lambda: post(block, 0, 1))

    loop(1, last, post_block)

    @pl.when(jnp.logical_not(collects))
    def _():
        pl.semaphore_wait(token, 1)

    post_block(last)
    first_stats[plane] = mine[...]

    @pl.when(home)
    def _():
        block = jnp.where(jnp.logical_and(lower, plane < last), last - 1 - plane, plane)
        recv[here] = send[block * slab]

    def wait_rows(ref, count, sem):
        some = ref.at[pl.ds(0, count)]
        pltpu.make_async_copy(some, some, sem).wait()

    def share(step):
        other = lax.rem(here + step, sources)
        return row_copy(
            last_stats.at[here], last_stats.at[here], sent, last_recv,
            plane * slab + other // lon_count, lax.rem(other, lon_count),
        )

    @pl.when(plane != last)
    def _():
        wait_rows(first_stats, planes - 1, stat_recv)
        last_stats[here] = jnp.max(first_stats[...], axis=0)
        loop(1, sources, lambda step: share(step).start())

    forward = row_copy(best, best, sent, best_recv, last * slab + x_pos, lon_pos)

    def finish_range():
        @pl.when(plane != last)
        def _():
            wait_rows(last_stats, sources - 1, last_recv)
            best[...] = jnp.max(last_stats[...], axis=0)

        pl.when(plane == last - 1)(forward.start)
        pl.when(plane == last)(lambda: pltpu.make_async_copy(best, best, best_recv).wait())
        for end in range(2):
            first = (end * levels + lat_pos) * fields
            line = jnp.broadcast_to(best[first // STRIP], (8, STRIP))
            line = pltpu.roll(line, lax.rem(STRIP - lax.rem(first, STRIP), STRIP), 1)
            line = line[:1, :fields]
            rng[end] = line if end == 0 else -line

    per_field = out.shape[0] // fields
    pairs = lon_count // 2
    crossed = lower == (lon_pos >= planes // 2)

    def drain():
        pl.when(plane == last - 1)(forward.wait_send)

        @pl.when(plane != last)
        def _():
            wait_rows(last_stats, sources - 1, sent)
            wait_rows(first_stats, last - 1, sent)

        pl.when(plane == last)(lambda: wait_rows(first_stats, last, sent))
        pl.when(home)(lambda: wait_rows(send, levels - 1, sent))
        unless(home, lambda: wait_rows(send, levels, sent))

    for turn in range(sources):
        core, i, j = 1 - turn // (pairs * slab), turn // pairs % slab, turn % pairs
        b = 2 * lax.rem(lon_pos // 2 + j, pairs) + core
        source = i * lon_count + b
        if turn == 0:
            pl.when(plane == last - 1)(finish_range)
        if turn == sources // 2:
            pl.when(jnp.logical_and(crossed, plane != last - 1))(finish_range)
        if turn == sources - 1:
            pl.when(jnp.logical_not(jnp.logical_or(crossed, plane == last - 1)))(finish_range)
            drain()
        unless(jnp.logical_and(home, source == here), lambda source=source: pltpu.make_async_copy(
            recv.at[source], recv.at[source], recv_sem.at[source]).wait())
        stage[source] = recv[source]
        rank = jnp.int32(0)
        for r in range(rows):
            live = mask[b, (lon_pos * slab + i) * rows + r]
            strip = stage[source, jnp.minimum(rank, slots - 1)]
            strip = jnp.where(live > 0, strip, 0.0)
            line = i * rows + r
            start = (line // 8 * lon_count + b) * 8 + line % 8
            out[pl.ds(start, fields, stride=per_field), :] = strip
            rank = rank + live


def store(history, record_range, history_out, record_range_out, sem):
    copies = [
        pltpu.make_async_copy(history.at[:, pl.ds(0, history_out.shape[1])], history_out, sem.at[0]),
        pltpu.make_async_copy(record_range, record_range_out, sem.at[1]),
    ]
    for copy in copies:
        copy.start()
    for copy in copies:
        copy.wait()


def per_device(fields, ocean_mask, scale_table, offset_table, scale_index, offset_index):
    nfield, levels, rows, cells = fields.shape
    lat_count = lax.axis_size("lat")
    lon_count = lax.axis_size("lon")
    slab = lat_count // lon_count
    slots = min(MAX_LIVE, rows)
    sources = slab * lon_count
    per_field = slab * rows * lon_count
    stat_rows = 2 * levels * nfield // STRIP
    hbm = pl.BlockSpec(memory_space=pltpu.HBM)
    vmem = pl.BlockSpec(memory_space=pltpu.VMEM)
    history, record_range = pl.pallas_call(
        functools.partial(exchange, (nfield, levels, rows, lat_count, lon_count)),
        out_shape=(
            pltpu.VMEM((nfield * (per_field + 8), STRIP), jnp.float32),
            pltpu.VMEM((2, 1, nfield), jnp.float32),
        ),
        in_specs=[hbm] * 6,
        out_specs=(vmem, vmem),
        scratch_shapes=[
            pltpu.SMEM((lon_count, lat_count * rows), jnp.int32),
            pltpu.SMEM(scale_table.shape, jnp.float32),
            pltpu.SMEM(offset_table.shape, jnp.float32),
            pltpu.SMEM(scale_index.shape, jnp.int32),
            pltpu.SMEM(offset_index.shape, jnp.int32),
            pltpu.SMEM((rows + 1,), jnp.int32),
            pltpu.VMEM((levels, rows, nfield, STRIP), jnp.float32),
            pltpu.VMEM((levels, slots, nfield, STRIP), jnp.float32),
            pltpu.VMEM((sources, slots, nfield, STRIP), jnp.float32),
            pltpu.VMEM((sources, slots, nfield, STRIP), jnp.float32),
            pltpu.VMEM((2 * levels * nfield, STRIP), jnp.float32),
            pltpu.VMEM((stat_rows, 1, STRIP), jnp.float32),
            pltpu.VMEM((lat_count // slab, stat_rows, 1, STRIP), jnp.float32),
            pltpu.VMEM((sources, stat_rows, 1, STRIP), jnp.float32),
            pltpu.VMEM((stat_rows, 1, STRIP), jnp.float32),
            pltpu.SemaphoreType.DMA,
            pltpu.SemaphoreType.DMA,
            pltpu.SemaphoreType.DMA,
            pltpu.SemaphoreType.DMA((sources,)),
            pltpu.SemaphoreType.DMA,
            pltpu.SemaphoreType.DMA,
            pltpu.SemaphoreType.DMA,
            pltpu.SemaphoreType.REGULAR,
            pltpu.SemaphoreType.REGULAR,
        ],
        compiler_params=pltpu.CompilerParams(
            collective_id=0, has_side_effects=True
        ),
    )(ocean_mask.T, scale_table, offset_table, scale_index, offset_index, fields)
    history, record_range = pl.pallas_call(
        store,
        out_shape=(
            jax.ShapeDtypeStruct((nfield, per_field, STRIP), jnp.float32),
            jax.ShapeDtypeStruct(record_range.shape, jnp.float32),
        ),
        in_specs=[vmem, vmem],
        out_specs=(hbm, hbm),
        scratch_shapes=[pltpu.SemaphoreType.DMA((2,))],
        compiler_params=pltpu.CompilerParams(vmem_limit_bytes=1 << 20),
    )(
        pltpu.with_memory_space_constraint(history.reshape(nfield, per_field + 8, STRIP), pltpu.VMEM),
        pltpu.with_memory_space_constraint(record_range, pltpu.VMEM),
    )
    history = history.reshape(nfield, slab * rows // 8, lon_count, 8, STRIP)
    history = history.transpose(0, 1, 3, 2, 4)
    return history.reshape(nfield, 1, slab * rows, lon_count * STRIP), record_range.reshape(2, nfield, 1)


def solution(mesh):
    return jax.shard_map(
        per_device,
        mesh=mesh,
        in_specs=(P(None, None, "lat", "lon"), P(), P(), P(), P(), P()),
        out_specs=(P(None, "lat", "lon", None), P(None, None, "lat")),
        check_vma=False,
    )
```

```python
import functools

import jax
import jax.numpy as jnp
from jax import lax
from jax.experimental import pallas as pl
from jax.experimental.pallas import tpu as pltpu
from jax.sharding import PartitionSpec as P

STRIP = 128
MAX_LIVE = 12
MESH = pl.DeviceIdType.MESH


def loop(low, high, body):
    def step(n, carry):
        body(n)
        return carry

    lax.fori_loop(low, high, step, 0)


def unless(condition, body):
    pl.when(jnp.logical_not(condition))(body)


def exchange(
    dims, mask_hbm, scale_table_hbm, offset_table_hbm, scale_index_hbm, offset_index_hbm, x_hbm,
    out, rng,
    mask, scale_table, offset_table, scale_index, offset_index, after,
    xs, send, recv, stage, part, mine, first_stats, last_stats, best,
    x_sem, in_sem, sent, recv_sem, stat_recv, last_recv, best_recv,
    token, cross,
):
    fields, levels, rows, lat_count, lon_count = dims
    slab = lat_count // lon_count
    planes = lat_count // slab
    sources = slab * lon_count
    slots = send.shape[1]
    last = planes - 1
    lat_pos = lax.axis_index("lat")
    lon_pos = lax.axis_index("lon")
    plane = lat_pos // slab
    here = lax.rem(lat_pos, slab) * lon_count + lon_pos
    lower = plane < planes // 2
    home = plane == lon_pos
    x_pos = lax.rem(lat_pos, slab)
    partner = lon_pos + 1 - 2 * lax.rem(lon_pos, 2)
    at_end = x_pos == slab - 1
    collects = jnp.logical_and(home, at_end)
    helps = jnp.logical_and(plane == partner, at_end)

    def place(block):
        early = jnp.where(lower, last - 1 - block, block)
        return jnp.where(block < last, early, last)

    def order(n):
        return place(n // slab) * slab + lax.rem(x_pos + lax.rem(n, slab), slab)

    barrier = pltpu.get_barrier_semaphore()

    def signal(sem, lat, lon):
        pl.semaphore_signal(sem, inc=1, device_id=(lat, lon), device_id_type=MESH)

    @pl.when(plane != last)
    def _():
        for b in range(lon_count):
            skip = jnp.logical_and(b == lon_pos, jnp.logical_or(home, at_end))
            unless(skip, lambda b=b: signal(barrier, lon_pos * slab + x_pos, b))

    @pl.when(plane != last)
    def _():
        for step in range(1, planes):
            signal(barrier, lax.rem(plane + step, planes) * slab + x_pos, lon_pos)

    smalls = [
        pltpu.make_async_copy(src, dst, in_sem)
        for n, (src, dst) in enumerate([
            (mask_hbm, mask), (scale_table_hbm, scale_table), (offset_table_hbm, offset_table),
            (scale_index_hbm, scale_index), (offset_index_hbm, offset_index),
        ])
    ]
    for copy in smalls:
        copy.start()
    for f in range(fields):
        pltpu.make_async_copy(x_hbm.at[f], xs.at[:, :, f], x_sem).start()
    for step in range(1, slab):
        signal(barrier, plane * slab + lax.rem(x_pos + step, slab), lon_pos)
    unless(jnp.logical_or(plane != last, collects), lambda: signal(barrier, lon_pos * slab + slab - 1, lon_pos))
    unless(collects, lambda: signal(barrier, plane * slab + slab - 1, plane))
    pl.when(collects)(lambda: signal(barrier, lat_pos, partner))

    for copy in smalls:
        copy.wait()

    following = first = jnp.int32(0)
    for r in reversed(range(rows)):
        first = jnp.where(mask[lon_pos, lat_pos * rows + r] > 0, r, first)
    following = first
    after[rows] = first
    for r in reversed(range(1, rows)):
        following = jnp.where(mask[lon_pos, lat_pos * rows + r] > 0, r, following)
        after[r] = following
    picks = [first]
    for k in range(1, slots):
        picks.append(after[picks[-1] + 1])

    which = lax.broadcasted_iota(jnp.int32, (fields, STRIP), 0)
    scales = jnp.zeros((fields, STRIP), jnp.float32)
    offsets = jnp.zeros((fields, STRIP), jnp.float32)
    for f in range(fields):
        scales = jnp.where(which == f, scale_table[scale_index[f]], scales)
        offsets = jnp.where(which == f, offset_table[offset_index[f]], offsets)

    pltpu.make_async_copy(xs, xs, x_sem).wait()
    for n in range(levels):
        level = order(n)
        high = low = None
        for k in range(slots):
            packed = (xs[level, picks[k]] - offsets) * scales
            send[n, k] = packed
            high = packed if k == 0 else jnp.maximum(high, packed)
            low = packed if k == 0 else jnp.minimum(low, packed)
        part[pl.ds(pl.multiple_of(level * fields, fields), fields), :] = high
        part[pl.ds(pl.multiple_of((levels + level) * fields, fields), fields), :] = -low

    for j in range(mine.shape[0]):
        tile = part[j * STRIP:(j + 1) * STRIP, :].T
        mine[j] = jnp.max(tile, axis=0, keepdims=True)

    inner = (plane != last).astype(jnp.int32)
    own = home.astype(jnp.int32)
    column = planes - 1 - inner
    calls = jnp.where(
        collects, slab - own * (1 - inner) + sources - 1, planes - 1 - own * inner + helps.astype(jnp.int32)
    )
    pl.semaphore_wait(barrier, column + slab - 1 + calls)

    def row_copy(src, dst, send, receive, lat, lon):
        return pltpu.make_async_remote_copy(
            src_ref=src, dst_ref=dst, send_sem=send, recv_sem=receive,
            device_id=(lat, lon), device_id_type=MESH,
        )

    def tell(other):
        return row_copy(
            mine, first_stats.at[plane], sent, stat_recv, other * slab + x_pos, lon_pos
        )

    def unless_here(other, body):
        unless(other == plane, body)

    @pl.when(collects)
    def _():
        def pass_on(step):
            other = lax.rem(here + step, sources)
            signal(token, plane * slab + other // lon_count, lax.rem(other, lon_count))

        loop(1, sources, pass_on)
        pl.semaphore_wait(token, 1)

    pl.when(helps)(lambda: signal(token, lat_pos, partner))
    for step in range(1, slab):
        signal(cross, plane * slab + lax.rem(x_pos + step, slab), lon_pos)

    loop(0, last, lambda other: unless_here(other, lambda: tell(other).start()))

    def remote(n):
        return pltpu.make_async_remote_copy(
            src_ref=send.at[n],
            dst_ref=recv.at[here],
            send_sem=sent,
            recv_sem=recv_sem.at[here],
            device_id=(order(n), plane),
            device_id_type=MESH,
        )

    def post(block, first, end):
        def start(i):
            n = block * slab + i
            unless(jnp.logical_and(order(n) == lat_pos, home), lambda: remote(n).start())

        loop(first, end, start)

    below = jnp.where(lower, last - plane, last)
    aside = jnp.logical_and(plane == planes // 2, jnp.logical_and(lax.rem(lon_pos, 2) == 0, at_end))
    unless(aside, lambda: post(0, 0, 1))
    loop(below, last, lambda block: post(block, 0, 1))
    pl.semaphore_wait(cross, slab - 1)
    post(0, 1, slab)
    pl.when(aside)(lambda: post(0, 0, 1))

    def post_block(block):
        post(block, 1, slab)
        unless(jnp.logical_and(block >= below, block < last), lambda: post(block, 0, 1))

    loop(1, last, post_block)

    @pl.when(jnp.logical_not(collects))
    def _():
        pl.semaphore_wait(token, 1)

    post_block(last)
    first_stats[plane] = mine[...]

    @pl.when(home)
    def _():
        block = jnp.where(jnp.logical_and(lower, plane < last), last - 1 - plane, plane)
        recv[here] = send[block * slab]

    def wait_rows(ref, count, sem):
        some = ref.at[pl.ds(0, count)]
        pltpu.make_async_copy(some, some, sem).wait()

    def share(step):
        other = lax.rem(here + step, sources)
        return row_copy(
            last_stats.at[here], last_stats.at[here], sent, last_recv,
            plane * slab + other // lon_count, lax.rem(other, lon_count),
        )

    @pl.when(plane != last)
    def _():
        wait_rows(first_stats, planes - 1, stat_recv)
        last_stats[here] = jnp.max(first_stats[...], axis=0)
        loop(1, sources, lambda step: share(step).start())

    forward = row_copy(best, best, sent, best_recv, last * slab + x_pos, lon_pos)

    def finish_range():
        @pl.when(plane != last)
        def _():
            wait_rows(last_stats, sources - 1, last_recv)
            best[...] = jnp.max(last_stats[...], axis=0)

        pl.when(plane == last - 1)(forward.start)
        pl.when(plane == last)(lambda: pltpu.make_async_copy(best, best, best_recv).wait())
        for end in range(2):
            first = (end * levels + lat_pos) * fields
            line = jnp.broadcast_to(best[first // STRIP], (8, STRIP))
            line = pltpu.roll(line, lax.rem(STRIP - lax.rem(first, STRIP), STRIP), 1)
            line = line[:1, :fields]
            rng[end] = line if end == 0 else -line

    per_field = out.shape[0] // fields
    pairs = lon_count // 2
    crossed = lower == (lon_pos >= planes // 2)

    def drain():
        pl.when(plane == last - 1)(forward.wait_send)

        @pl.when(plane != last)
        def _():
            wait_rows(last_stats, sources - 1, sent)
            wait_rows(first_stats, last - 1, sent)

        pl.when(plane == last)(lambda: wait_rows(first_stats, last, sent))
        pl.when(home)(lambda: wait_rows(send, levels - 1, sent))
        unless(home, lambda: wait_rows(send, levels, sent))

    for turn in range(sources):
        core, i, j = 1 - turn // (pairs * slab), turn // pairs % slab, turn % pairs
        b = 2 * lax.rem(lon_pos // 2 + j, pairs) + core
        source = i * lon_count + b
        if turn == 0:
            pl.when(plane == last - 1)(finish_range)
        if turn == sources // 2:
            pl.when(jnp.logical_and(crossed, plane != last - 1))(finish_range)
        if turn == sources - 1:
            pl.when(jnp.logical_not(jnp.logical_or(crossed, plane == last - 1)))(finish_range)
            drain()
        unless(jnp.logical_and(home, source == here), lambda source=source: pltpu.make_async_copy(
            recv.at[source], recv.at[source], recv_sem.at[source]).wait())
        stage[source] = recv[source]
        rank = jnp.int32(0)
        for r in range(rows):
            live = mask[b, (lon_pos * slab + i) * rows + r]
            strip = stage[source, jnp.minimum(rank, slots - 1)]
            strip = jnp.where(live > 0, strip, 0.0)
            line = i * rows + r
            start = (line // 8 * lon_count + b) * 8 + line % 8
            out[pl.ds(start, fields, stride=per_field), :] = strip
            rank = rank + live


def store(history, record_range, history_out, record_range_out, sem):
    copies = [
        pltpu.make_async_copy(history.at[:, pl.ds(0, history_out.shape[1])], history_out, sem.at[0]),
        pltpu.make_async_copy(record_range, record_range_out, sem.at[1]),
    ]
    for copy in copies:
        copy.start()
    for copy in copies:
        copy.wait()


def per_device(fields, ocean_mask, scale_table, offset_table, scale_index, offset_index):
    nfield, levels, rows, cells = fields.shape
    lat_count = lax.axis_size("lat")
    lon_count = lax.axis_size("lon")
    slab = lat_count // lon_count
    slots = min(MAX_LIVE, rows)
    sources = slab * lon_count
    per_field = slab * rows * lon_count
    stat_rows = 2 * levels * nfield // STRIP
    hbm = pl.BlockSpec(memory_space=pltpu.HBM)
    vmem = pl.BlockSpec(memory_space=pltpu.VMEM)
    history, record_range = pl.pallas_call(
        functools.partial(exchange, (nfield, levels, rows, lat_count, lon_count)),
        out_shape=(
            pltpu.VMEM((nfield * (per_field + 8), STRIP), jnp.float32),
            pltpu.VMEM((2, 1, nfield), jnp.float32),
        ),
        in_specs=[hbm] * 6,
        out_specs=(vmem, vmem),
        scratch_shapes=[
            pltpu.SMEM((lon_count, lat_count * rows), jnp.int32),
            pltpu.SMEM(scale_table.shape, jnp.float32),
            pltpu.SMEM(offset_table.shape, jnp.float32),
            pltpu.SMEM(scale_index.shape, jnp.int32),
            pltpu.SMEM(offset_index.shape, jnp.int32),
            pltpu.SMEM((rows + 1,), jnp.int32),
            pltpu.VMEM((levels, rows, nfield, STRIP), jnp.float32),
            pltpu.VMEM((levels, slots, nfield, STRIP), jnp.float32),
            pltpu.VMEM((sources, slots, nfield, STRIP), jnp.float32),
            pltpu.VMEM((sources, slots, nfield, STRIP), jnp.float32),
            pltpu.VMEM((2 * levels * nfield, STRIP), jnp.float32),
            pltpu.VMEM((stat_rows, 1, STRIP), jnp.float32),
            pltpu.VMEM((lat_count // slab, stat_rows, 1, STRIP), jnp.float32),
            pltpu.VMEM((sources, stat_rows, 1, STRIP), jnp.float32),
            pltpu.VMEM((stat_rows, 1, STRIP), jnp.float32),
            pltpu.SemaphoreType.DMA,
            pltpu.SemaphoreType.DMA,
            pltpu.SemaphoreType.DMA,
            pltpu.SemaphoreType.DMA((sources,)),
            pltpu.SemaphoreType.DMA,
            pltpu.SemaphoreType.DMA,
            pltpu.SemaphoreType.DMA,
            pltpu.SemaphoreType.REGULAR,
            pltpu.SemaphoreType.REGULAR,
        ],
        compiler_params=pltpu.CompilerParams(
            collective_id=0, has_side_effects=True
        ),
    )(ocean_mask.T, scale_table, offset_table, scale_index, offset_index, fields)
    history, record_range = pl.pallas_call(
        store,
        out_shape=(
            jax.ShapeDtypeStruct((nfield, per_field, STRIP), jnp.float32),
            jax.ShapeDtypeStruct(record_range.shape, jnp.float32),
        ),
        in_specs=[vmem, vmem],
        out_specs=(hbm, hbm),
        scratch_shapes=[pltpu.SemaphoreType.DMA((2,))],
        compiler_params=pltpu.CompilerParams(vmem_limit_bytes=1 << 20),
    )(
        pltpu.with_memory_space_constraint(history.reshape(nfield, per_field + 8, STRIP), pltpu.VMEM),
        pltpu.with_memory_space_constraint(record_range, pltpu.VMEM),
    )
    history = history.reshape(nfield, slab * rows // 8, lon_count, 8, STRIP)
    history = history.transpose(0, 1, 3, 2, 4)
    return history.reshape(nfield, 1, slab * rows, lon_count * STRIP), record_range.reshape(2, nfield, 1)


def solution(mesh):
    return jax.shard_map(
        per_device,
        mesh=mesh,
        in_specs=(P(None, None, "lat", "lon"), P(), P(), P(), P(), P()),
        out_specs=(P(None, "lat", "lon", None), P(None, None, "lat")),
        check_vma=False,
    )
```

```python
import functools

import jax
import jax.numpy as jnp
from jax import lax
from jax.experimental import pallas as pl
from jax.experimental.pallas import tpu as pltpu
from jax.sharding import PartitionSpec as P

STRIP = 128
MAX_LIVE = 12
MESH = pl.DeviceIdType.MESH


def loop(low, high, body):
    def step(n, carry):
        body(n)
        return carry

    lax.fori_loop(low, high, step, 0)


def unless(condition, body):
    pl.when(jnp.logical_not(condition))(body)


def exchange(
    dims, mask_hbm, scale_table_hbm, offset_table_hbm, scale_index_hbm, offset_index_hbm, x_hbm,
    out, rng,
    mask, scale_table, offset_table, scale_index, offset_index, after,
    xs, send, recv, stage, part, mine, first_stats, last_stats, best,
    x_sem, in_sem, sent, recv_sem, stat_recv, last_recv, best_recv,
    token, cross,
):
    fields, levels, rows, lat_count, lon_count = dims
    slab = lat_count // lon_count
    planes = lat_count // slab
    sources = slab * lon_count
    slots = send.shape[1]
    last = planes - 1
    lat_pos = lax.axis_index("lat")
    lon_pos = lax.axis_index("lon")
    plane = lat_pos // slab
    here = lax.rem(lat_pos, slab) * lon_count + lon_pos
    lower = plane < planes // 2
    home = plane == lon_pos
    x_pos = lax.rem(lat_pos, slab)
    partner = lon_pos + 1 - 2 * lax.rem(lon_pos, 2)
    at_end = x_pos == slab - 1
    collects = jnp.logical_and(home, at_end)
    helps = jnp.logical_and(plane == partner, at_end)

    def place(block):
        early = jnp.where(lower, last - 1 - block, block)
        return jnp.where(block < last, early, last)

    def order(n):
        return place(n // slab) * slab + lax.rem(x_pos + lax.rem(n, slab), slab)

    barrier = pltpu.get_barrier_semaphore()

    def signal(sem, lat, lon):
        pl.semaphore_signal(sem, inc=1, device_id=(lat, lon), device_id_type=MESH)

    @pl.when(plane != last)
    def _():
        for b in range(lon_count):
            skip = jnp.logical_and(b == lon_pos, jnp.logical_or(home, at_end))
            unless(skip, lambda b=b: signal(barrier, lon_pos * slab + x_pos, b))

    @pl.when(plane != last)
    def _():
        for step in range(1, planes):
            signal(barrier, lax.rem(plane + step, planes) * slab + x_pos, lon_pos)

    smalls = [
        pltpu.make_async_copy(src, dst, in_sem)
        for n, (src, dst) in enumerate([
            (mask_hbm, mask), (scale_table_hbm, scale_table), (offset_table_hbm, offset_table),
            (scale_index_hbm, scale_index), (offset_index_hbm, offset_index),
        ])
    ]
    for copy in smalls:
        copy.start()
    for f in range(fields):
        pltpu.make_async_copy(x_hbm.at[f], xs.at[:, :, f], x_sem).start()
    for step in range(1, slab):
        signal(barrier, plane * slab + lax.rem(x_pos + step, slab), lon_pos)
    unless(jnp.logical_or(plane != last, collects), lambda: signal(barrier, lon_pos * slab + slab - 1, lon_pos))
    unless(collects, lambda: signal(barrier, plane * slab + slab - 1, plane))
    pl.when(collects)(lambda: signal(barrier, lat_pos, partner))

    for copy in smalls:
        copy.wait()

    following = first = jnp.int32(0)
    for r in reversed(range(rows)):
        first = jnp.where(mask[lon_pos, lat_pos * rows + r] > 0, r, first)
    following = first
    after[rows] = first
    for r in reversed(range(1, rows)):
        following = jnp.where(mask[lon_pos, lat_pos * rows + r] > 0, r, following)
        after[r] = following
    picks = [first]
    for k in range(1, slots):
        picks.append(after[picks[-1] + 1])

    which = lax.broadcasted_iota(jnp.int32, (fields, STRIP), 0)
    scales = jnp.zeros((fields, STRIP), jnp.float32)
    offsets = jnp.zeros((fields, STRIP), jnp.float32)
    for f in range(fields):
        scales = jnp.where(which == f, scale_table[scale_index[f]], scales)
        offsets = jnp.where(which == f, offset_table[offset_index[f]], offsets)

    pltpu.make_async_copy(xs, xs, x_sem).wait()
    for n in range(levels):
        level = order(n)
        high = low = None
        for k in range(slots):
            packed = (xs[level, picks[k]] - offsets) * scales
            send[n, k] = packed
            high = packed if k == 0 else jnp.maximum(high, packed)
            low = packed if k == 0 else jnp.minimum(low, packed)
        part[pl.ds(pl.multiple_of(level * fields, fields), fields), :] = high
        part[pl.ds(pl.multiple_of((levels + level) * fields, fields), fields), :] = -low

    for j in range(mine.shape[0]):
        tile = part[j * STRIP:(j + 1) * STRIP, :].T
        mine[j] = jnp.max(tile, axis=0, keepdims=True)

    inner = (plane != last).astype(jnp.int32)
    own = home.astype(jnp.int32)
    column = planes - 1 - inner
    calls = jnp.where(
        collects, slab - own * (1 - inner) + sources - 1, planes - 1 - own * inner + helps.astype(jnp.int32)
    )
    pl.semaphore_wait(barrier, column + slab - 1 + calls)

    def row_copy(src, dst, send, receive, lat, lon):
        return pltpu.make_async_remote_copy(
            src_ref=src, dst_ref=dst, send_sem=send, recv_sem=receive,
            device_id=(lat, lon), device_id_type=MESH,
        )

    def tell(other):
        return row_copy(
            mine, first_stats.at[plane], sent, stat_recv, other * slab + x_pos, lon_pos
        )

    def unless_here(other, body):
        unless(other == plane, body)

    @pl.when(collects)
    def _():
        def pass_on(step):
            other = lax.rem(here + step, sources)
            signal(token, plane * slab + other // lon_count, lax.rem(other, lon_count))

        loop(1, sources, pass_on)
        pl.semaphore_wait(token, 1)

    pl.when(helps)(lambda: signal(token, lat_pos, partner))
    for step in range(1, slab):
        signal(cross, plane * slab + lax.rem(x_pos + step, slab), lon_pos)

    loop(0, last, lambda other: unless_here(other, lambda: tell(other).start()))

    def remote(n):
        return pltpu.make_async_remote_copy(
            src_ref=send.at[n],
            dst_ref=recv.at[here],
            send_sem=sent,
            recv_sem=recv_sem.at[here],
            device_id=(order(n), plane),
            device_id_type=MESH,
        )

    def post(block, first, end):
        def start(i):
            n = block * slab + i
            unless(jnp.logical_and(order(n) == lat_pos, home), lambda: remote(n).start())

        loop(first, end, start)

    below = jnp.where(lower, last - plane, last)
    aside = jnp.logical_and(plane == planes // 2, jnp.logical_and(lax.rem(lon_pos, 2) == 0, at_end))
    unless(aside, lambda: post(0, 0, 1))
    loop(below, last, lambda block: post(block, 0, 1))
    pl.semaphore_wait(cross, slab - 1)
    post(0, 1, slab)
    pl.when(aside)(lambda: post(0, 0, 1))

    def post_block(block):
        post(block, 1, slab)
        unless(jnp.logical_and(block >= below, block < last), lambda: post(block, 0, 1))

    loop(1, last, post_block)

    @pl.when(jnp.logical_not(collects))
    def _():
        pl.semaphore_wait(token, 1)

    post_block(last)
    first_stats[plane] = mine[...]

    @pl.when(home)
    def _():
        block = jnp.where(jnp.logical_and(lower, plane < last), last - 1 - plane, plane)
        recv[here] = send[block * slab]

    def wait_rows(ref, count, sem):
        some = ref.at[pl.ds(0, count)]
        pltpu.make_async_copy(some, some, sem).wait()

    def share(step):
        other = lax.rem(here + step, sources)
        return row_copy(
            last_stats.at[here], last_stats.at[here], sent, last_recv,
            plane * slab + other // lon_count, lax.rem(other, lon_count),
        )

    @pl.when(plane != last)
    def _():
        wait_rows(first_stats, planes - 1, stat_recv)
        last_stats[here] = jnp.max(first_stats[...], axis=0)
        loop(1, sources, lambda step: share(step).start())

    forward = row_copy(best, best, sent, best_recv, last * slab + x_pos, lon_pos)

    def finish_range():
        @pl.when(plane != last)
        def _():
            wait_rows(last_stats, sources - 1, last_recv)
            best[...] = jnp.max(last_stats[...], axis=0)

        pl.when(plane == last - 1)(forward.start)
        pl.when(plane == last)(lambda: pltpu.make_async_copy(best, best, best_recv).wait())
        for end in range(2):
            first = (end * levels + lat_pos) * fields
            line = jnp.broadcast_to(best[first // STRIP], (8, STRIP))
            line = pltpu.roll(line, lax.rem(STRIP - lax.rem(first, STRIP), STRIP), 1)
            line = line[:1, :fields]
            rng[end] = line if end == 0 else -line

    pairs = lon_count // 2
    crossed = lower == (lon_pos >= planes // 2)

    def drain():
        pl.when(plane == last - 1)(forward.wait_send)

        @pl.when(plane != last)
        def _():
            wait_rows(last_stats, sources - 1, sent)
            wait_rows(first_stats, last - 1, sent)

        pl.when(plane == last)(lambda: wait_rows(first_stats, last, sent))
        pl.when(home)(lambda: wait_rows(send, levels - 1, sent))
        unless(home, lambda: wait_rows(send, levels, sent))

    for turn in range(sources):
        core, j, i = 1 - turn // (pairs * slab), turn // slab % pairs, turn % slab
        b = 2 * lax.rem(lon_pos // 2 + j, pairs) + core
        source = i * lon_count + b
        if turn == 0:
            pl.when(plane == last - 1)(finish_range)
        if turn == sources // 2:
            pl.when(jnp.logical_and(crossed, plane != last - 1))(finish_range)
        if turn == sources - 1:
            pl.when(jnp.logical_not(jnp.logical_or(crossed, plane == last - 1)))(finish_range)
            drain()
        unless(jnp.logical_and(home, source == here), lambda source=source: pltpu.make_async_copy(
            recv.at[source], recv.at[source], recv_sem.at[source]).wait())
        stage[source] = recv[source]
        rank = jnp.int32(0)
        for r in range(rows):
            live = mask[b, (lon_pos * slab + i) * rows + r]
            strip = stage[source, jnp.minimum(rank, slots - 1)]
            strip = jnp.where(live > 0, strip, 0.0)
            line = i * rows + r
            start = (line // 8 * lon_count + b) * 8 + line % 8
            out[start] = strip
            rank = rank + live


def store(history, record_range, history_out, record_range_out, sem):
    copies = [
        pltpu.make_async_copy(history.at[:, f], history_out.at[f], sem.at[0])
        for f in range(history_out.shape[0])
    ]
    copies.append(pltpu.make_async_copy(record_range, record_range_out, sem.at[1]))
    for copy in copies:
        copy.start()
    pltpu.make_async_copy(history, history, sem.at[0]).wait()
    copies[-1].wait()


def per_device(fields, ocean_mask, scale_table, offset_table, scale_index, offset_index):
    nfield, levels, rows, cells = fields.shape
    lat_count = lax.axis_size("lat")
    lon_count = lax.axis_size("lon")
    slab = lat_count // lon_count
    slots = min(MAX_LIVE, rows)
    sources = slab * lon_count
    per_field = slab * rows * lon_count
    stat_rows = 2 * levels * nfield // STRIP
    hbm = pl.BlockSpec(memory_space=pltpu.HBM)
    vmem = pl.BlockSpec(memory_space=pltpu.VMEM)
    history, record_range = pl.pallas_call(
        functools.partial(exchange, (nfield, levels, rows, lat_count, lon_count)),
        out_shape=(
            pltpu.VMEM((per_field, nfield, STRIP), jnp.float32),
            pltpu.VMEM((2, 1, nfield), jnp.float32),
        ),
        in_specs=[hbm] * 6,
        out_specs=(vmem, vmem),
        scratch_shapes=[
            pltpu.SMEM((lon_count, lat_count * rows), jnp.int32),
            pltpu.SMEM(scale_table.shape, jnp.float32),
            pltpu.SMEM(offset_table.shape, jnp.float32),
            pltpu.SMEM(scale_index.shape, jnp.int32),
            pltpu.SMEM(offset_index.shape, jnp.int32),
            pltpu.SMEM((rows + 1,), jnp.int32),
            pltpu.VMEM((levels, rows, nfield, STRIP), jnp.float32),
            pltpu.VMEM((levels, slots, nfield, STRIP), jnp.float32),
            pltpu.VMEM((sources, slots, nfield, STRIP), jnp.float32),
            pltpu.VMEM((sources, slots, nfield, STRIP), jnp.float32),
            pltpu.VMEM((2 * levels * nfield, STRIP), jnp.float32),
            pltpu.VMEM((stat_rows, 1, STRIP), jnp.float32),
            pltpu.VMEM((lat_count // slab, stat_rows, 1, STRIP), jnp.float32),
            pltpu.VMEM((sources, stat_rows, 1, STRIP), jnp.float32),
            pltpu.VMEM((stat_rows, 1, STRIP), jnp.float32),
            pltpu.SemaphoreType.DMA,
            pltpu.SemaphoreType.DMA,
            pltpu.SemaphoreType.DMA,
            pltpu.SemaphoreType.DMA((sources,)),
            pltpu.SemaphoreType.DMA,
            pltpu.SemaphoreType.DMA,
            pltpu.SemaphoreType.DMA,
            pltpu.SemaphoreType.REGULAR,
            pltpu.SemaphoreType.REGULAR,
        ],
        compiler_params=pltpu.CompilerParams(
            collective_id=0, has_side_effects=True
        ),
    )(ocean_mask.T, scale_table, offset_table, scale_index, offset_index, fields)
    history, record_range = pl.pallas_call(
        store,
        out_shape=(
            jax.ShapeDtypeStruct((nfield, per_field, STRIP), jnp.float32),
            jax.ShapeDtypeStruct(record_range.shape, jnp.float32),
        ),
        in_specs=[vmem, vmem],
        out_specs=(hbm, hbm),
        scratch_shapes=[pltpu.SemaphoreType.DMA((2,))],
        compiler_params=pltpu.CompilerParams(vmem_limit_bytes=1 << 20),
    )(
        pltpu.with_memory_space_constraint(history, pltpu.VMEM),
        pltpu.with_memory_space_constraint(record_range, pltpu.VMEM),
    )
    history = history.reshape(nfield, slab * rows // 8, lon_count, 8, STRIP)
    history = history.transpose(0, 1, 3, 2, 4)
    return history.reshape(nfield, 1, slab * rows, lon_count * STRIP), record_range.reshape(2, nfield, 1)


def solution(mesh):
    return jax.shard_map(
        per_device,
        mesh=mesh,
        in_specs=(P(None, None, "lat", "lon"), P(), P(), P(), P(), P()),
        out_specs=(P(None, "lat", "lon", None), P(None, None, "lat")),
        check_vma=False,
    )
```
